32 devices in a mesh: blk: 8 (over z, core), section: 4 (over y, x).
Axes of the slice: x: 2, y: 2, z: 4, core: 2. Of those that a mesh axis runs over, the one named last changes fastest.
Arguments:
- hidden: bfloat16 [4, 2048, 4096], P('section', 'blk'), parts along dimension 1, may hold values from -6 to 6
- exit_layer: int32 [4096], P('blk'), parts along dimension 0, may hold values from 1 to 2
- lengths: int32 [4096], P('blk'), parts along dimension 0, may hold values from 1 to 16, as said below
- kv_cache: bfloat16 [4, 2048, 16, 256], P('section', 'blk'), parts along dimension 1, may hold values from -256 to 256
- norm_gain: bfloat16 [4, 4096], P('section'), may hold values from 0.5 to 1.5
- w_qkv: bfloat16 [4, 4096, 1280], P('section'), may hold values from -0.0625 to 0.0625
- w_out: bfloat16 [4, 1024, 4096], P('section'), may hold values from -0.1875 to 0.1875
Outputs:
- settled: bfloat16 [4096, 8192], P('blk', 'section'), parts along dimension 0
The draws below stay inside these ranges and needn't reach their ends.
There are 8 independent parts, one for each index of `blk`. The reference program is written for one: setup_inputs(seed, part) draws one part's arguments, and reference() takes and returns one part's arrays. A program takes and returns all parts, laid end to end along the dimension named above; an argument that names none is the same for every part. Nothing has to cross between parts.
Inputs may be any that keep to these rules, and one draw needn't show every extreme that they name: `lengths`: some token has length 16.
All inputs are finite; a program needn't handle non-finite values.
Results may differ from the reference program's by a relative error of at most 0.03.
Values may be sent and summed in bfloat16 or wider, within the bound.
No kernel may reach another device: no remote copies, remote signals or barrier semaphores. Data moves between devices by JAX's collectives and lax.ppermute only.
A program may use at most 64 MiB of HBM per device.

```python
import jax
import jax.numpy as jnp
from jax import lax

D = 8192
HD = 128
QH = 8
BLOCK = 64
MICRO = 8
CTX = 16
SHARDS = 2
LAYERS = 2
TOKENS = 512


def draw_exit_layer(key, part):
    count_key = jax.random.fold_in(key, 11)
    order_key = jax.random.fold_in(key, 13)
    depth_key = jax.random.fold_in(key, 14)
    counts = jax.random.randint(count_key, (MICRO,), BLOCK // 4, BLOCK // 2 + 1)
    scores = jax.random.randint(order_key, (MICRO, BLOCK), 0, 1 << 20) * BLOCK + jnp.arange(BLOCK)[None, :]
    ranking = jnp.argsort(jnp.argsort(scores, axis=1), axis=1)
    deeper = ranking < counts[:, None]
    depth = jax.random.randint(depth_key, (MICRO, BLOCK), 2, LAYERS + 1)
    return jnp.where(deeper, depth, 1).reshape(-1).astype(jnp.int32)


def draw_lengths(key, part):
    length_key = jax.random.fold_in(key, 21)
    forced_key = jax.random.fold_in(key, 22)
    drawn = jax.random.randint(length_key, (TOKENS,), 1, CTX + 1)
    forced = jax.random.randint(forced_key, (), 0, TOKENS)
    return jnp.where(jnp.arange(TOKENS) == forced, CTX, drawn).astype(jnp.int32)


def draw_kv_cache(key, part):
    keys_key = jax.random.fold_in(key, 31)
    values_key = jax.random.fold_in(key, 32)
    shape = (SHARDS * LAYERS, TOKENS // SHARDS, CTX, HD)
    keys = jax.random.truncated_normal(keys_key, -4.0, 4.0, shape, jnp.float32)
    values = jax.random.truncated_normal(values_key, -4.0, 4.0, shape, jnp.float32)
    return jnp.concatenate([keys, values], axis=-1).astype(jnp.bfloat16)


def steps_of(key, dims, cuts, low, largest):
    def one(dim, shards_of):
        draws = jax.random.uniform(jax.random.fold_in(jax.random.fold_in(key, 6), dim), (shards_of,), jnp.float32, low / len(cuts), largest / len(cuts))
        return jnp.repeat(jnp.exp(draws), dims[dim] // shards_of).reshape((-1,) + (1,) * (len(dims) - dim - 1))

    loudness = one(*cuts[0])
    for cut in cuts[1:]:
        loudness = loudness * one(*cut)
    return loudness


def centred(stream_key, extent, spread, limit, shards=(), held_as=jnp.bfloat16):
    values = spread * jax.random.normal(stream_key, extent, jnp.float32)
    if shards:
        values = values * steps_of(stream_key, extent, shards, -0.22, 0.18)
    return jnp.clip(values, -limit, limit).astype(held_as)


def setup_inputs(seed: int = 0, part: int = 0) -> dict:
    arg_keys = jax.random.split(jax.random.key(seed), 8)
    own_keys = jax.random.split(jax.random.fold_in(arg_keys[7], part), 8)
    hidden = centred(own_keys[0], (SHARDS * LAYERS, TOKENS // LAYERS, D // SHARDS), 1.0, 6.0, ((0, 4),))
    exit_layer = draw_exit_layer(jax.random.fold_in(jax.random.fold_in(arg_keys[7], part), 71), part)
    lengths = draw_lengths(jax.random.fold_in(jax.random.fold_in(arg_keys[7], part), 71), part)
    kv_cache = draw_kv_cache(jax.random.fold_in(jax.random.fold_in(arg_keys[7], part), 71), part)
    norm_gain = jnp.clip(1.0 + 0.1 * jax.random.normal(arg_keys[4], (SHARDS * LAYERS, D // SHARDS), jnp.float32), 0.5, 1.5).astype(jnp.bfloat16)
    w_qkv = centred(arg_keys[5], (SHARDS * LAYERS, D // SHARDS, (QH + 2) * HD), D ** -0.5, 0.0625, ((0, 4),))
    w_out = centred(arg_keys[6], (SHARDS * LAYERS, QH * HD, D // SHARDS), (QH * HD) ** -0.5, 0.1875, ((0, 4),))
    return dict(hidden=hidden, exit_layer=exit_layer, lengths=lengths, kv_cache=kv_cache, norm_gain=norm_gain, w_qkv=w_qkv, w_out=w_out)


EPSILON = 1e-05
NEGATIVE = -1e+30

def attend(state, active, len_rows, cache_rows, gain_row, proj_weight, out_weight):
    query_width = out_weight.shape[0]
    head_size = (proj_weight.shape[1] - query_width) // 2
    heads = query_width // head_size
    rows = state.shape[0]
    context = cache_rows.shape[1]
    widened = state.astype(jnp.float32)
    scaled = (widened * gain_row.astype(jnp.float32)).astype(jnp.bfloat16)
    mean_square = lax.optimization_barrier(jnp.mean(widened * widened, axis=-1))
    projected = jnp.dot(scaled, proj_weight, preferred_element_type=jnp.float32) * lax.rsqrt(mean_square + EPSILON)[:, None]
    query = (projected[:, :query_width] * (1.0 / jnp.sqrt(jnp.float32(head_size)))).astype(jnp.bfloat16)
    query = query.reshape(rows, heads, head_size).astype(jnp.float32)
    key_new = projected[:, query_width:query_width + head_size].astype(jnp.bfloat16).astype(jnp.float32)
    value_new = projected[:, query_width + head_size:].astype(jnp.bfloat16).astype(jnp.float32)
    keys = cache_rows[:, :, :head_size].astype(jnp.float32)
    values = cache_rows[:, :, head_size:].astype(jnp.float32)
    scores = jnp.einsum('rhd,rcd->rhc', query, keys)
    own = jnp.einsum('rhd,rd->rh', query, key_new)
    positions = jnp.arange(context, dtype=jnp.int32)
    usable = (positions[None, :] < len_rows[:, None])[:, None, :]
    scores = jnp.where(usable, scores, NEGATIVE)
    row_top = jnp.maximum(lax.optimization_barrier(jnp.max(scores, axis=-1)), own)
    raw = jnp.where(usable, jnp.exp(scores - row_top[:, :, None]), jnp.float32(0.0))
    raw_own = jnp.exp(own - row_top)
    total = lax.optimization_barrier(jnp.sum(raw, axis=-1)) + raw_own
    weights = (raw / total[:, :, None]).astype(jnp.bfloat16).astype(jnp.float32)
    own_weight = (raw_own / total).astype(jnp.bfloat16).astype(jnp.float32)
    attended = jnp.einsum('rhc,rcd->rhd', weights, values) + own_weight[:, :, None] * value_new[:, None, :]
    attended = attended.astype(jnp.bfloat16).reshape(rows, query_width)
    branch_out = jnp.dot(attended, out_weight, preferred_element_type=jnp.float32)
    updated = (widened + branch_out).astype(jnp.bfloat16)
    return jnp.where(active[:, None], updated, state)

def reference(hidden, exit_layer, lengths, kv_cache, norm_gain, w_qkv, w_out):
    group = BLOCK // SHARDS
    span = D // (SHARDS * LAYERS)
    columns = w_qkv.shape[2]
    query_width = w_out.shape[1]
    width = kv_cache.shape[3]
    rounds = MICRO // LAYERS
    gains = norm_gain.reshape(LAYERS, SHARDS, LAYERS, span).transpose(0, 2, 1, 3).reshape(LAYERS, D)
    projections = w_qkv.reshape(LAYERS, SHARDS, LAYERS, span, columns).transpose(0, 2, 1, 3, 4).reshape(LAYERS, D, columns)
    outputs = w_out.reshape(LAYERS, SHARDS, query_width, LAYERS, span).transpose(0, 2, 3, 1, 4).reshape(LAYERS, query_width, D)
    cache = kv_cache.reshape(LAYERS, SHARDS, MICRO, group, CTX, width).transpose(0, 2, 1, 3, 4, 5).reshape(LAYERS, MICRO * BLOCK, CTX, width)
    arranged = hidden.reshape(LAYERS, SHARDS, rounds, BLOCK, LAYERS, span).transpose(2, 0, 3, 4, 1, 5).reshape(rounds, LAYERS, BLOCK, D)
    arranged = jnp.stack([arranged[:, (LAYERS - place) % LAYERS] for place in range(LAYERS)], axis=1)
    state = arranged.reshape(MICRO * BLOCK, D)
    for layer in range(LAYERS):
        state = attend(state, exit_layer > layer, lengths, cache[layer], gains[layer], projections[layer], outputs[layer])
    return state
```

```python
import functools
import math

import jax
import jax.numpy as jnp
from jax import lax
from jax.experimental import pallas as pl
from jax.experimental.pallas import tpu as pltpu
from jax.sharding import PartitionSpec as P

BLOCK = 64
MICRO = 8


EPSILON = 1e-05
NEGATIVE = -1e30


def partner(value, axis, distance):
    return lax.ppermute(value, axis, [(i, i ^ 1 << distance) for i in range(lax.axis_size(axis))])


def shifted(value, axis, steps):
    count = lax.axis_size(axis)
    pairs = [(source, (source + steps) % count) for source in range(count)]
    return lax.ppermute(value, axis, pairs)


def body(hidden, exit_layer, lengths, kv_cache, norm_gain, w_qkv, w_out):
    devices = lax.axis_size("section")
    index = lax.axis_index("section")
    shards = max(2, devices // 4)
    cycle_size = devices // shards
    segment_bits = cycle_size.bit_length() - 1
    shard_bits = shards.bit_length() - 1
    segment_index = index // shards
    shard_index = index % shards
    own_blocks = hidden[0]
    gain_row = norm_gain[0].astype(jnp.float32)
    proj_weight = w_qkv[0]
    out_weight = w_out[0]
    cache_all = kv_cache[0]
    query_width = out_weight.shape[0]
    head_size = (proj_weight.shape[1] - query_width) // 2
    heads = query_width // head_size
    quarter = proj_weight.shape[0]
    total_width = quarter * shards
    group_rows = BLOCK // shards
    rounds = MICRO // cycle_size
    context = cache_all.shape[1]
    positions = jnp.arange(context, dtype=jnp.int32)
    blank_block = jnp.zeros((BLOCK, quarter), jnp.bfloat16)

    def advance(carry, microstep):
        incoming, arriving, records = carry
        micro_index = microstep - segment_index
        in_range = (micro_index >= 0) & (micro_index < MICRO)
        slot = jnp.clip(micro_index, 0, MICRO - 1)
        on_turn = microstep % cycle_size == 0
        local_slot = jnp.minimum(microstep // cycle_size, rounds - 1)
        own_block = lax.dynamic_slice_in_dim(own_blocks, local_slot * BLOCK, BLOCK, 0)
        exit_rows = lax.dynamic_slice_in_dim(exit_layer, slot * BLOCK, BLOCK)
        own_lengths = lax.dynamic_slice_in_dim(
            lengths, slot * BLOCK + shard_index * group_rows, group_rows
        )
        own_cache = lax.dynamic_slice_in_dim(cache_all, slot * group_rows, group_rows, 0)
        first_input = jnp.where(on_turn, own_block, arriving)
        entering = jnp.where(segment_index == 0, first_input, incoming)
        active = exit_rows > segment_index
        gate = in_range & (jnp.sum(active.astype(jnp.int32)) > 0)

        def local_partials():
            widened = entering.astype(jnp.float32)
            scaled = (widened * gain_row).astype(jnp.bfloat16)
            return (
                jnp.dot(scaled, proj_weight, preferred_element_type=jnp.float32),
                jnp.sum(widened * widened, axis=1),
            )

        def no_partials():
            return (
                jnp.zeros((BLOCK, proj_weight.shape[1]), jnp.float32),
                jnp.zeros((BLOCK,), jnp.float32),
            )

        partial_proj, partial_squares = lax.cond(gate, local_partials, no_partials)
        kept = (partial_proj, partial_squares)
        for level in range(shard_bits):
            bit = shard_bits - 1 - level
            upper = index >> bit & 1
            halves = tuple(
                (piece.reshape((2, piece.shape[0] // 2) + piece.shape[1:]) for piece in kept)
            )
            keep = tuple((jnp.where(upper == 1, half[1], half[0]) for half in halves))
            send = tuple((jnp.where(upper == 1, half[0], half[1]) for half in halves))
            received = partner(send, "section", bit)
            kept = tuple((first + second for first, second in zip(keep, received)))
        own_proj, own_squares = kept

        def local_attention():
            fitted = own_proj * lax.rsqrt(own_squares / total_width + EPSILON)[:, None]
            query = (fitted[:, :query_width] * (1.0 / math.sqrt(head_size))).astype(jnp.bfloat16)
            query = query.reshape(group_rows, heads, head_size)
            key_new = fitted[:, query_width : query_width + head_size].astype(jnp.bfloat16)
            value_new = fitted[:, query_width + head_size :].astype(jnp.bfloat16)
            scores = jnp.einsum(
                "rhd,rcd->rhc",
                query,
                own_cache[:, :, :head_size],
                preferred_element_type=jnp.float32,
            )
            own = jnp.einsum("rhd,rd->rh", query, key_new, preferred_element_type=jnp.float32)
            usable = (positions[None, :] < own_lengths[:, None])[:, None, :]
            scores = jnp.where(usable, scores, NEGATIVE)
            row_top = jnp.maximum(jnp.max(scores, axis=-1), own)
            raw = jnp.where(usable, jnp.exp(scores - row_top[:, :, None]), jnp.float32(0.0))
            raw_own = jnp.exp(own - row_top)
            total = jnp.sum(raw, axis=-1) + raw_own
            weights = (raw / total[:, :, None]).astype(jnp.bfloat16)
            own_weight = (raw_own / total).astype(jnp.bfloat16)
            attended = jnp.einsum(
                "rhc,rcd->rhd",
                weights,
                own_cache[:, :, head_size:],
                preferred_element_type=jnp.float32,
            )
            attended = (
                attended
                + own_weight.astype(jnp.float32)[:, :, None]
                * value_new.astype(jnp.float32)[:, None, :]
            )
            return attended.astype(jnp.bfloat16).reshape(group_rows, query_width)

        def no_attention():
            return jnp.zeros((group_rows, query_width), jnp.bfloat16)

        collected = lax.cond(gate, local_attention, no_attention)
        for level in range(shard_bits):
            bit = level
            other = partner(collected, "section", bit)
            upper = index >> bit & 1
            collected = jnp.where(
                upper == 1,
                jnp.concatenate([other, collected], 0),
                jnp.concatenate([collected, other], 0),
            )

        def local_update():
            branch_out = jnp.dot(collected, out_weight, preferred_element_type=jnp.float32)
            updated = (entering.astype(jnp.float32) + branch_out).astype(jnp.bfloat16)
            return jnp.where(active[:, None], updated, entering)

        def keep_state():
            return entering

        outgoing = lax.cond(gate, local_update, keep_state)
        leaving = in_range & (exit_rows == segment_index + 1)
        previous = lax.dynamic_slice_in_dim(records, slot * BLOCK, BLOCK, 0)
        records = lax.dynamic_update_slice_in_dim(
            records, jnp.where(leaving[:, None], outgoing, previous), slot * BLOCK, 0
        )
        relayed = jnp.where(on_turn & (segment_index > 0), own_block, arriving)
        incoming, arriving = shifted((outgoing, relayed), "section", shards)
        return ((incoming, arriving, records), None)

    start = (blank_block, blank_block, jnp.zeros((MICRO * BLOCK, quarter), jnp.bfloat16))
    carry, _ = lax.scan(advance, start, jnp.arange(MICRO + cycle_size - 1, dtype=jnp.int32))
    kept = carry[2]
    for level in range(segment_bits):
        bit = shard_bits + segment_bits - 1 - level
        upper = index >> bit & 1
        halves = kept.reshape(kept.shape[0], 2, kept.shape[1] // 2)
        keep = jnp.where(upper == 1, halves[:, 1], halves[:, 0])
        send = jnp.where(upper == 1, halves[:, 0], halves[:, 1])
        received = partner(send, "section", bit)
        kept = (keep.astype(jnp.float32) + received.astype(jnp.float32)).astype(jnp.bfloat16)
    return kept


def project_kernel(place, xa_ref, xb_ref, gain_ref, w_ref, keep_ref, keep_sq_ref, send_ref, acc_ref, sq_ref):
    step = pl.program_id(0)
    upper = place[0]
    shard = place[1]
    x = jnp.where(upper == 0, xa_ref[...], xb_ref[...]).astype(jnp.float32)
    scaled = (x * gain_ref[...].astype(jnp.float32)).astype(jnp.bfloat16)
    product = jnp.dot(scaled, w_ref[...], preferred_element_type=jnp.float32)
    squares = x * x
    folded = squares[:, :128]
    for lane in range(128, squares.shape[1], 128):
        folded = folded + squares[:, lane : lane + 128]

    @pl.when(step == 0)
    def _():
        acc_ref[...] = product
        sq_ref[...] = folded

    @pl.when(step > 0)
    def _():
        acc_ref[...] += product
        sq_ref[...] += folded

    @pl.when(step == pl.num_programs(0) - 1)
    def _():
        group = BLOCK // 2
        width = keep_ref.shape[1]
        for block in range(acc_ref.shape[0] // BLOCK):
            here = pl.ds(pl.multiple_of(block * BLOCK + shard * group, group), group)
            there = pl.ds(pl.multiple_of(block * BLOCK + (1 - shard) * group, group), group)
            rows = pl.ds(block * group, group)
            keep_ref[rows, :] = acc_ref[here, :]
            send_ref[rows, :width] = acc_ref[there, :].astype(jnp.bfloat16)
            own = jnp.sum(sq_ref[here, :], axis=1, keepdims=True)
            keep_sq_ref[rows, :] = jnp.broadcast_to(own, (group, 128))
            other = jnp.broadcast_to(jnp.sum(sq_ref[there, :], axis=1, keepdims=True), (group, 128))
            high = other.astype(jnp.bfloat16)
            low = (other - high.astype(jnp.float32)).astype(jnp.bfloat16)
            lanes = lax.broadcasted_iota(jnp.int32, (group, 128), 1)
            pair = jnp.where(lanes < 64, high.astype(jnp.float32), low.astype(jnp.float32))
            send_ref[rows, width:] = pair.astype(jnp.bfloat16)


def project(place, xa, xb, gain, w):
    rows, features = xa.shape
    width = w.shape[1]
    tile = min(512, features)
    steps = features // tile
    half = rows // 2
    return pl.pallas_call(
        project_kernel,
        grid_spec=pltpu.PrefetchScalarGridSpec(
            num_scalar_prefetch=1,
            grid=(steps,),
            in_specs=[
                pl.BlockSpec((rows, tile), lambda k, p: (0, jnp.where(p[0] == 0, k, 0))),
                pl.BlockSpec((rows, tile), lambda k, p: (0, jnp.where(p[0] == 0, 0, k))),
                pl.BlockSpec((1, tile), lambda k, p: (0, k)),
                pl.BlockSpec((tile, width), lambda k, p: (k, 0)),
            ],
            out_specs=[
                pl.BlockSpec((half, width), lambda k, p: (0, 0)),
                pl.BlockSpec((half, 128), lambda k, p: (0, 0)),
                pl.BlockSpec((half, width + 128), lambda k, p: (0, 0)),
            ],
            scratch_shapes=[
                pltpu.VMEM((rows, width), jnp.float32),
                pltpu.VMEM((rows, 128), jnp.float32),
            ],
        ),
        out_shape=[
            jax.ShapeDtypeStruct((half, width), jnp.float32),
            jax.ShapeDtypeStruct((half, 128), jnp.float32),
            jax.ShapeDtypeStruct((half, width + 128), jnp.bfloat16),
        ],
        cost_estimate=pl.CostEstimate(
            flops=2 * rows * features * width,
            bytes_accessed=2 * features * width + 4 * rows * features,
            transcendentals=0,
        ),
        name="project",
    )(place, xa, xb, gain, w)


def attend_kernel(total_width, place, keep_ref, keep_sq_ref, recv_ref, kv0_ref, kv1_ref, len0_ref, len1_ref, out_ref):
    width = keep_ref.shape[1]
    head_size = kv0_ref.shape[3] // 2
    context = kv0_ref.shape[2]
    heads = width // head_size - 2
    group = BLOCK // 2
    tokens = 16
    columns = tokens * context
    other = recv_ref[:, width:].astype(jnp.float32)
    squares = keep_sq_ref[:, :1] + other[:, :1] + other[:, 64:65]
    factor = lax.rsqrt(squares / total_width + EPSILON)
    fitted = (keep_ref[...] + recv_ref[:, :width].astype(jnp.float32)) * factor
    scale = 1.0 / math.sqrt(head_size)
    row = lax.broadcasted_iota(jnp.int32, (heads * tokens, columns), 0)
    column = lax.broadcasted_iota(jnp.int32, (heads * tokens, columns), 1)
    same = (row % tokens) == (column // context)
    position = lax.broadcasted_iota(jnp.int32, (1, columns), 1) % context
    for block, (kv_ref, len_ref) in enumerate(((kv0_ref, len0_ref), (kv1_ref, len1_ref))):
        for part in range(group // tokens):
            base = block * group + part * tokens
            rows = slice(base, base + tokens)
            span = slice(part * tokens, (part + 1) * tokens)
            query = jnp.concatenate(
                [fitted[rows, h * head_size : (h + 1) * head_size] for h in range(heads)], axis=0
            )
            query = (query * scale).astype(jnp.bfloat16)
            key_new = fitted[rows, heads * head_size : (heads + 1) * head_size].astype(jnp.bfloat16)
            value_new = fitted[rows, (heads + 1) * head_size :].astype(jnp.bfloat16)
            key_new = jnp.concatenate([key_new.astype(jnp.float32)] * heads, axis=0)
            value_new = jnp.concatenate([value_new.astype(jnp.float32)] * heads, axis=0)
            keys = kv_ref[0, span, :, :head_size].reshape(columns, head_size)
            values = kv_ref[0, span, :, head_size:].reshape(columns, head_size)
            scores = lax.dot_general(
                query, keys, (((1,), (1,)), ((), ())), preferred_element_type=jnp.float32
            )
            own = jnp.sum(query.astype(jnp.float32) * key_new, axis=1, keepdims=True)
            usable = same & (position < len_ref[0, part : part + 1, :])
            scores = jnp.where(usable, scores, NEGATIVE)
            row_top = jnp.maximum(jnp.max(scores, axis=1, keepdims=True), own)
            raw = jnp.where(usable, jnp.exp(scores - row_top), 0.0)
            raw_own = jnp.exp(own - row_top)
            total = jnp.sum(raw, axis=1, keepdims=True) + raw_own
            weights = (raw / total).astype(jnp.bfloat16)
            own_weight = (raw_own / total).astype(jnp.bfloat16).astype(jnp.float32)
            attended = jnp.dot(weights, values, preferred_element_type=jnp.float32)
            attended = (attended + own_weight * value_new).astype(jnp.bfloat16)
            for h in range(heads):
                out_ref[rows, h * head_size : (h + 1) * head_size] = attended[
                    h * tokens : (h + 1) * tokens
                ]


def attend(total_width, where_kv, keep, keep_sq, recv, kv, lens, query_width):
    half, width = keep.shape
    kv_block = (1,) + kv.shape[1:]
    len_block = (1,) + lens.shape[1:]
    return pl.pallas_call(
        functools.partial(attend_kernel, total_width),
        grid_spec=pltpu.PrefetchScalarGridSpec(
            num_scalar_prefetch=1,
            grid=(1,),
            in_specs=[
                pl.BlockSpec((half, width), lambda i, p: (0, 0)),
                pl.BlockSpec((half, 128), lambda i, p: (0, 0)),
                pl.BlockSpec((half, width + 128), lambda i, p: (0, 0)),
                pl.BlockSpec(kv_block, lambda i, p: (p[0], 0, 0, 0)),
                pl.BlockSpec(kv_block, lambda i, p: (p[1], 0, 0, 0)),
                pl.BlockSpec(len_block, lambda i, p: (p[0], 0, 0)),
                pl.BlockSpec(len_block, lambda i, p: (p[1], 0, 0)),
            ],
            out_specs=pl.BlockSpec((half, query_width), lambda i, p: (0, 0)),
        ),
        out_shape=jax.ShapeDtypeStruct((half, query_width), jnp.bfloat16),
        cost_estimate=pl.CostEstimate(
            flops=900_000_000, bytes_accessed=2 * 2 * math.prod(kv_block), transcendentals=0
        ),
        name="attend",
    )(where_kv, keep, keep_sq, recv, kv, kv, lens, lens)


def output_kernel(place, own_ref, recv_ref, active_ref, xa_ref, xb_ref, w_ref, out_ref, att_ref):
    step = pl.program_id(0)
    upper = place[0]
    shard = place[1]

    @pl.when(step == 0)
    def _():
        group = BLOCK // 2
        for block in range(att_ref.shape[0] // BLOCK):
            here = pl.ds(pl.multiple_of(block * BLOCK + shard * group, group), group)
            there = pl.ds(pl.multiple_of(block * BLOCK + (1 - shard) * group, group), group)
            rows = pl.ds(block * group, group)
            att_ref[here, :] = own_ref[rows, :]
            att_ref[there, :] = recv_ref[rows, :]

    branch = jnp.dot(att_ref[...], w_ref[...], preferred_element_type=jnp.float32)
    state = jnp.where(upper == 0, xa_ref[...], xb_ref[...]).astype(jnp.float32)
    out_ref[...] = jnp.where(active_ref[...] > 0, state + branch, state).astype(jnp.bfloat16)


def output(place, own, recv, active, xa, xb, w):
    rows, features = xa.shape
    depth = w.shape[0]
    tile = min(512, features)
    return pl.pallas_call(
        output_kernel,
        grid_spec=pltpu.PrefetchScalarGridSpec(
            num_scalar_prefetch=1,
            grid=(features // tile,),
            in_specs=[
                pl.BlockSpec(own.shape, lambda n, p: (0, 0)),
                pl.BlockSpec(recv.shape, lambda n, p: (0, 0)),
                pl.BlockSpec(active.shape, lambda n, p: (0, 0)),
                pl.BlockSpec((rows, tile), lambda n, p: (0, jnp.where(p[0] == 0, n, 0))),
                pl.BlockSpec((rows, tile), lambda n, p: (0, jnp.where(p[0] == 0, 0, n))),
                pl.BlockSpec((depth, tile), lambda n, p: (0, n)),
            ],
            out_specs=pl.BlockSpec((rows, tile), lambda n, p: (0, n)),
            scratch_shapes=[pltpu.VMEM((rows, depth), jnp.bfloat16)],
        ),
        out_shape=jax.ShapeDtypeStruct((rows, features), jnp.bfloat16),
        cost_estimate=pl.CostEstimate(
            flops=2 * rows * features * depth,
            bytes_accessed=2 * features * depth + 6 * rows * features,
            transcendentals=0,
        ),
        name="output",
    )(place, own, recv, active, xa, xb, w)


def paired_body(hidden, exit_layer, lengths, kv_cache, norm_gain, w_qkv, w_out):
    index = lax.axis_index("section")
    upper = index // 2
    shard = index % 2
    swap = [(i, i ^ 1) for i in range(4)]
    up = [(0, 2), (1, 3)]
    down = [(2, 0), (3, 1)]
    states = hidden[0]
    gain = norm_gain
    proj_weight = w_qkv[0]
    out_weight = w_out[0]
    features = proj_weight.shape[0]
    group = BLOCK // 2
    context = kv_cache.shape[2]
    tall = 2 * BLOCK
    count = MICRO // 2
    kv = kv_cache[0].reshape((MICRO, group) + kv_cache.shape[2:])
    own_lengths = lax.dynamic_index_in_dim(lengths.reshape(MICRO, 2, group), shard, 1, False)
    lens = jnp.repeat(own_lengths, context, axis=1).reshape(MICRO, group // 16, 16 * context)
    place = jnp.stack([upper, shard]).astype(jnp.int32)
    active = (exit_layer > upper).astype(jnp.int32).reshape(MICRO, BLOCK)

    def blocks_of(chunk):
        first = 4 * (chunk % 2) + chunk // 2
        return first, first + 2

    moved = [
        lax.ppermute(states[c * tall : (c + 1) * tall], "section", down) for c in range(count // 2)
    ]
    zero = states[:tall]
    arrived = []
    finals = []
    for step in range(count + 2):
        lower_chunk = min(step, count - 1)
        upper_chunk = max(step - 2, 0)
        if step < 2:
            xa = states[step * tall : (step + 1) * tall]
            xb = xa
        elif step < count:
            xa = moved[step - 2]
            xb = arrived[step - 2]
        else:
            xb = arrived[step - 2]
            xa = xb
        low = blocks_of(lower_chunk)
        high = blocks_of(upper_chunk)
        picks = jnp.where(upper == 0, jnp.array(low, jnp.int32), jnp.array(high, jnp.int32))
        keep, keep_sq, send = project(place, xa, xb, gain, proj_weight)
        received = lax.ppermute(send, "section", swap)
        own = attend(float(2 * features), picks, keep, keep_sq, received, kv, lens, out_weight.shape[0])
        other = lax.ppermute(own, "section", swap)
        chunk_active = jnp.where(
            upper == 0,
            jnp.concatenate([active[m] for m in low]),
            jnp.concatenate([active[m] for m in high]),
        )
        state = output(place, own, other, chunk_active[:, None], xa, xb, out_weight)
        if step < count:
            arrived.append(lax.ppermute(state, "section", up))
        if step >= 2:
            settled = lax.ppermute(state[:, : features // 2], "section", down)
            finals.append(jnp.where(upper == 0, settled, state[:, features // 2 :]))
    pieces = [None] * MICRO
    for chunk in range(count):
        for place_in, block in enumerate(blocks_of(chunk)):
            pieces[block] = finals[chunk][place_in * BLOCK : (place_in + 1) * BLOCK]
    return jnp.concatenate(pieces, axis=0)


def solution(mesh):
    paired = mesh.shape["section"] == 4
    return jax.shard_map(
        paired_body if paired else body,
        mesh=mesh,
        in_specs=(
            P("section", "blk", None),
            P("blk"),
            P("blk"),
            P("section", "blk", None, None),
            P("section", None),
            P("section", None, None),
            P("section", None, None),
        ),
        out_specs=P("blk", "section"),
        check_vma=False,
    )
```

```python
import functools
import math

import jax
import jax.numpy as jnp
from jax import lax
from jax.experimental import pallas as pl
from jax.experimental.pallas import tpu as pltpu
from jax.sharding import PartitionSpec as P

BLOCK = 64
MICRO = 8


EPSILON = 1e-05
NEGATIVE = -1e30


def partner(value, axis, distance):
    return lax.ppermute(value, axis, [(i, i ^ 1 << distance) for i in range(lax.axis_size(axis))])


def shifted(value, axis, steps):
    count = lax.axis_size(axis)
    pairs = [(source, (source + steps) % count) for source in range(count)]
    return lax.ppermute(value, axis, pairs)


def body(hidden, exit_layer, lengths, kv_cache, norm_gain, w_qkv, w_out):
    devices = lax.axis_size("section")
    index = lax.axis_index("section")
    shards = max(2, devices // 4)
    cycle_size = devices // shards
    segment_bits = cycle_size.bit_length() - 1
    shard_bits = shards.bit_length() - 1
    segment_index = index // shards
    shard_index = index % shards
    own_blocks = hidden[0]
    gain_row = norm_gain[0].astype(jnp.float32)
    proj_weight = w_qkv[0]
    out_weight = w_out[0]
    cache_all = kv_cache[0]
    query_width = out_weight.shape[0]
    head_size = (proj_weight.shape[1] - query_width) // 2
    heads = query_width // head_size
    quarter = proj_weight.shape[0]
    total_width = quarter * shards
    group_rows = BLOCK // shards
    rounds = MICRO // cycle_size
    context = cache_all.shape[1]
    positions = jnp.arange(context, dtype=jnp.int32)
    blank_block = jnp.zeros((BLOCK, quarter), jnp.bfloat16)

    def advance(carry, microstep):
        incoming, arriving, records = carry
        micro_index = microstep - segment_index
        in_range = (micro_index >= 0) & (micro_index < MICRO)
        slot = jnp.clip(micro_index, 0, MICRO - 1)
        on_turn = microstep % cycle_size == 0
        local_slot = jnp.minimum(microstep // cycle_size, rounds - 1)
        own_block = lax.dynamic_slice_in_dim(own_blocks, local_slot * BLOCK, BLOCK, 0)
        exit_rows = lax.dynamic_slice_in_dim(exit_layer, slot * BLOCK, BLOCK)
        own_lengths = lax.dynamic_slice_in_dim(
            lengths, slot * BLOCK + shard_index * group_rows, group_rows
        )
        own_cache = lax.dynamic_slice_in_dim(cache_all, slot * group_rows, group_rows, 0)
        first_input = jnp.where(on_turn, own_block, arriving)
        entering = jnp.where(segment_index == 0, first_input, incoming)
        active = exit_rows > segment_index
        gate = in_range & (jnp.sum(active.astype(jnp.int32)) > 0)

        def local_partials():
            widened = entering.astype(jnp.float32)
            scaled = (widened * gain_row).astype(jnp.bfloat16)
            return (
                jnp.dot(scaled, proj_weight, preferred_element_type=jnp.float32),
                jnp.sum(widened * widened, axis=1),
            )

        def no_partials():
            return (
                jnp.zeros((BLOCK, proj_weight.shape[1]), jnp.float32),
                jnp.zeros((BLOCK,), jnp.float32),
            )

        partial_proj, partial_squares = lax.cond(gate, local_partials, no_partials)
        kept = (partial_proj, partial_squares)
        for level in range(shard_bits):
            bit = shard_bits - 1 - level
            upper = index >> bit & 1
            halves = tuple(
                (piece.reshape((2, piece.shape[0] // 2) + piece.shape[1:]) for piece in kept)
            )
            keep = tuple((jnp.where(upper == 1, half[1], half[0]) for half in halves))
            send = tuple((jnp.where(upper == 1, half[0], half[1]) for half in halves))
            received = partner(send, "section", bit)
            kept = tuple((first + second for first, second in zip(keep, received)))
        own_proj, own_squares = kept

        def local_attention():
            fitted = own_proj * lax.rsqrt(own_squares / total_width + EPSILON)[:, None]
            query = (fitted[:, :query_width] * (1.0 / math.sqrt(head_size))).astype(jnp.bfloat16)
            query = query.reshape(group_rows, heads, head_size)
            key_new = fitted[:, query_width : query_width + head_size].astype(jnp.bfloat16)
            value_new = fitted[:, query_width + head_size :].astype(jnp.bfloat16)
            scores = jnp.einsum(
                "rhd,rcd->rhc",
                query,
                own_cache[:, :, :head_size],
                preferred_element_type=jnp.float32,
            )
            own = jnp.einsum("rhd,rd->rh", query, key_new, preferred_element_type=jnp.float32)
            usable = (positions[None, :] < own_lengths[:, None])[:, None, :]
            scores = jnp.where(usable, scores, NEGATIVE)
            row_top = jnp.maximum(jnp.max(scores, axis=-1), own)
            raw = jnp.where(usable, jnp.exp(scores - row_top[:, :, None]), jnp.float32(0.0))
            raw_own = jnp.exp(own - row_top)
            total = jnp.sum(raw, axis=-1) + raw_own
            weights = (raw / total[:, :, None]).astype(jnp.bfloat16)
            own_weight = (raw_own / total).astype(jnp.bfloat16)
            attended = jnp.einsum(
                "rhc,rcd->rhd",
                weights,
                own_cache[:, :, head_size:],
                preferred_element_type=jnp.float32,
            )
            attended = (
                attended
                + own_weight.astype(jnp.float32)[:, :, None]
                * value_new.astype(jnp.float32)[:, None, :]
            )
            return attended.astype(jnp.bfloat16).reshape(group_rows, query_width)

        def no_attention():
            return jnp.zeros((group_rows, query_width), jnp.bfloat16)

        collected = lax.cond(gate, local_attention, no_attention)
        for level in range(shard_bits):
            bit = level
            other = partner(collected, "section", bit)
            upper = index >> bit & 1
            collected = jnp.where(
                upper == 1,
                jnp.concatenate([other, collected], 0),
                jnp.concatenate([collected, other], 0),
            )

        def local_update():
            branch_out = jnp.dot(collected, out_weight, preferred_element_type=jnp.float32)
            updated = (entering.astype(jnp.float32) + branch_out).astype(jnp.bfloat16)
            return jnp.where(active[:, None], updated, entering)

        def keep_state():
            return entering

        outgoing = lax.cond(gate, local_update, keep_state)
        leaving = in_range & (exit_rows == segment_index + 1)
        previous = lax.dynamic_slice_in_dim(records, slot * BLOCK, BLOCK, 0)
        records = lax.dynamic_update_slice_in_dim(
            records, jnp.where(leaving[:, None], outgoing, previous), slot * BLOCK, 0
        )
        relayed = jnp.where(on_turn & (segment_index > 0), own_block, arriving)
        incoming, arriving = shifted((outgoing, relayed), "section", shards)
        return ((incoming, arriving, records), None)

    start = (blank_block, blank_block, jnp.zeros((MICRO * BLOCK, quarter), jnp.bfloat16))
    carry, _ = lax.scan(advance, start, jnp.arange(MICRO + cycle_size - 1, dtype=jnp.int32))
    kept = carry[2]
    for level in range(segment_bits):
        bit = shard_bits + segment_bits - 1 - level
        upper = index >> bit & 1
        halves = kept.reshape(kept.shape[0], 2, kept.shape[1] // 2)
        keep = jnp.where(upper == 1, halves[:, 1], halves[:, 0])
        send = jnp.where(upper == 1, halves[:, 0], halves[:, 1])
        received = partner(send, "section", bit)
        kept = (keep.astype(jnp.float32) + received.astype(jnp.float32)).astype(jnp.bfloat16)
    return kept


LIMIT = 10 * 1024 * 1024


def vmem(shape, dtype):
    return pltpu.VMEM(shape, dtype)


IN_VMEM = pl.BlockSpec(memory_space=pltpu.VMEM)
IN_SMEM = pl.BlockSpec(memory_space=pltpu.SMEM)
ANYWHERE = pl.BlockSpec(memory_space=pl.ANY)


def split_kernel(x_ref, *refs):
    outs, sem = refs[:-1], refs[-1]
    tall = outs[0].shape[0]
    copies = [
        pltpu.make_async_copy(x_ref.at[i * tall : (i + 1) * tall], out, sem.at[i])
        for i, out in enumerate(outs)
    ]
    for copy in copies:
        copy.start()
    for copy in copies:
        copy.wait()


def split(x, tall):
    pieces = x.shape[0] // tall
    return pl.pallas_call(
        split_kernel,
        in_specs=[ANYWHERE],
        out_specs=[IN_VMEM] * pieces,
        out_shape=[vmem((tall, x.shape[1]), x.dtype)] * pieces,
        scratch_shapes=[pltpu.SemaphoreType.DMA((pieces,))],
        compiler_params=pltpu.CompilerParams(vmem_limit_bytes=LIMIT),
        cost_estimate=pl.CostEstimate(flops=10**9, bytes_accessed=2 * x.size, transcendentals=0),
        name="split",
    )(x)


def groups_first(x):
    group = BLOCK // 2
    order = [b * BLOCK + s * group for s in range(2) for b in range(x.shape[0] // BLOCK)]
    return jnp.concatenate([x[row : row + group] for row in order], axis=0)


def project_kernel(slices, place, xa_ref, xb_ref, gain_ref, w_ref, *refs):
    if slices:
        keep_ref, keep_sq_ref, send_ref, held_ref, acc_ref, sq_ref, sem = refs
        depth = w_ref.shape[0] // slices
        copies = [
            pltpu.make_async_copy(
                w_ref.at[i * depth : (i + 1) * depth], held_ref.at[i * depth : (i + 1) * depth], sem.at[i]
            )
            for i in range(slices)
        ]
        for copy in copies:
            copy.start()
    elif len(refs) == 8:
        other_ref, keep_ref, keep_sq_ref, send_ref, held_ref, acc_ref, sq_ref, sem = refs
        copy = pltpu.make_async_copy(other_ref, held_ref, sem.at[0])
        copy.start()
    else:
        keep_ref, keep_sq_ref, send_ref, acc_ref, sq_ref = refs
    upper = place[0]
    shard = place[1]
    features = xa_ref.shape[1]
    pieces = slices if slices else 4
    depth = features // pieces
    squares = None
    for i in range(pieces):
        columns = slice(i * depth, (i + 1) * depth)
        x = jnp.where(upper == 0, xa_ref[:, columns], xb_ref[:, columns]).astype(jnp.float32)
        for lane in range(0, depth, 128):
            part = x[:, lane : lane + 128]
            squares = part * part if squares is None else squares + part * part
        scaled = (x * gain_ref[:, columns].astype(jnp.float32)).astype(jnp.bfloat16)
        if slices:
            copies[i].wait()
            weight = held_ref[columns, :]
        else:
            weight = w_ref[columns, :]
        product = jnp.dot(scaled, weight, preferred_element_type=jnp.float32)
        if i == 0:
            acc_ref[...] = product
        else:
            acc_ref[...] += product
    sq_ref[...] = squares
    group = BLOCK // 2
    width = keep_ref.shape[1]
    for block in range(acc_ref.shape[0] // BLOCK):
        here = pl.ds(pl.multiple_of(block * BLOCK + shard * group, group), group)
        there = pl.ds(pl.multiple_of(block * BLOCK + (1 - shard) * group, group), group)
        rows = pl.ds(block * group, group)
        keep_ref[rows, :] = acc_ref[here, :]
        send_ref[rows, :width] = acc_ref[there, :].astype(jnp.bfloat16)
        own = jnp.sum(sq_ref[here, :], axis=1, keepdims=True)
        keep_sq_ref[rows, :] = jnp.broadcast_to(own, (group, 128))
        other = jnp.broadcast_to(jnp.sum(sq_ref[there, :], axis=1, keepdims=True), (group, 128))
        high = other.astype(jnp.bfloat16)
        low = (other - high.astype(jnp.float32)).astype(jnp.bfloat16)
        lanes = lax.broadcasted_iota(jnp.int32, (group, 128), 1)
        pair = jnp.where(lanes < 64, high.astype(jnp.float32), low.astype(jnp.float32))
        send_ref[rows, width:] = pair.astype(jnp.bfloat16)
    if not slices and len(refs) == 8:
        copy.wait()


def project(place, xa, xb, gain, w, load=False, extra=None):
    rows, features = xa.shape
    width = w.shape[1]
    half = rows // 2
    slices = 4 if load else 0
    held = w if load else extra
    inputs = [place, xa, xb, gain, w] + ([] if extra is None else [extra])
    outs = [
        vmem((half, width), jnp.float32),
        vmem((half, 128), jnp.float32),
        vmem((half, width + 128), jnp.bfloat16),
    ]
    scratch = [pltpu.VMEM((rows, width), jnp.float32), pltpu.VMEM((rows, 128), jnp.float32)]
    if held is not None:
        outs.append(vmem(held.shape, held.dtype))
        scratch.append(pltpu.SemaphoreType.DMA((4,)))
    return pl.pallas_call(
        functools.partial(project_kernel, slices),
        in_specs=[IN_SMEM, IN_VMEM, IN_VMEM, IN_VMEM, ANYWHERE if load else IN_VMEM]
        + ([] if extra is None else [ANYWHERE]),
        out_specs=[IN_VMEM] * len(outs),
        out_shape=outs,
        scratch_shapes=scratch,
        compiler_params=pltpu.CompilerParams(vmem_limit_bytes=LIMIT),
        cost_estimate=pl.CostEstimate(
            flops=2 * rows * features * width,
            bytes_accessed=2 * features * width + 4 * rows * features,
            transcendentals=0,
        ),
        name="project",
    )(*inputs)


def attend_kernel(total_width, picks, keep_ref, keep_sq_ref, recv_ref, kv_ref, len_ref, out_ref):
    width = keep_ref.shape[1]
    context = kv_ref.shape[1]
    head_size = kv_ref.shape[2] // 2
    heads = width // head_size - 2
    group = BLOCK // 2
    tokens = 16
    columns = tokens * context
    other = recv_ref[:, width:].astype(jnp.float32)
    squares = keep_sq_ref[:, :1] + other[:, :1] + other[:, 64:65]
    factor = lax.rsqrt(squares / total_width + EPSILON)
    scale = 1.0 / math.sqrt(head_size)
    row = lax.broadcasted_iota(jnp.int32, (heads * tokens, columns), 0)
    column = lax.broadcasted_iota(jnp.int32, (heads * tokens, columns), 1)
    same = (row % tokens) == (column // context)
    position = lax.broadcasted_iota(jnp.int32, (1, columns), 1) % context
    pieces = [(block, part) for block in range(2) for part in range(group // tokens)]
    fitted, queries, tops, masks, all_scores, owns = [], [], [], [], [], []
    for block, part in pieces:
        base = block * group + part * tokens
        rows = slice(base, base + tokens)
        fit = (keep_ref[rows, :] + recv_ref[rows, :width].astype(jnp.float32)) * factor[rows]
        query = jnp.concatenate(
            [fit[:, h * head_size : (h + 1) * head_size] for h in range(heads)], axis=0
        )
        fitted.append(fit[:, heads * head_size :])
        queries.append((query * scale).astype(jnp.bfloat16))
    for i, (block, part) in enumerate(pieces):
        first = pl.multiple_of(picks[block] * group + part * tokens, tokens)
        keys = kv_ref[pl.ds(first, tokens), :, :head_size].reshape(columns, head_size)
        all_scores.append(
            lax.dot_general(
                queries[i], keys, (((1,), (1,)), ((), ())), preferred_element_type=jnp.float32
            )
        )
        key_new = fitted[i][:, :head_size].astype(jnp.bfloat16).astype(jnp.float32)
        key_new = jnp.concatenate([key_new] * heads, axis=0)
        owns.append(jnp.sum(queries[i].astype(jnp.float32) * key_new, axis=1, keepdims=True))
    for i, (block, part) in enumerate(pieces):
        limit = len_ref[picks[block], part : part + 1, :]
        masks.append(same & (position < limit))
        all_scores[i] = jnp.where(masks[i], all_scores[i], NEGATIVE)
        tops.append(jnp.maximum(jnp.max(all_scores[i], axis=1, keepdims=True), owns[i]))
    raws, raw_owns, totals = [], [], []
    for i in range(len(pieces)):
        raws.append(jnp.where(masks[i], jnp.exp(all_scores[i] - tops[i]), 0.0))
        raw_owns.append(jnp.exp(owns[i] - tops[i]))
        totals.append(jnp.sum(raws[i], axis=1, keepdims=True) + raw_owns[i])
    for i, (block, part) in enumerate(pieces):
        base = block * group + part * tokens
        first = pl.multiple_of(picks[block] * group + part * tokens, tokens)
        values = kv_ref[pl.ds(first, tokens), :, head_size:].reshape(columns, head_size)
        weights = (raws[i] / totals[i]).astype(jnp.bfloat16)
        own_weight = (raw_owns[i] / totals[i]).astype(jnp.bfloat16).astype(jnp.float32)
        value_new = fitted[i][:, head_size:].astype(jnp.bfloat16).astype(jnp.float32)
        value_new = jnp.concatenate([value_new] * heads, axis=0)
        attended = jnp.dot(weights, values, preferred_element_type=jnp.float32)
        attended = (attended + own_weight * value_new).astype(jnp.bfloat16)
        for h in range(heads):
            out_ref[base : base + tokens, h * head_size : (h + 1) * head_size] = attended[
                h * tokens : (h + 1) * tokens
            ]


def attend(total_width, picks, keep, keep_sq, recv, kv, lens, query_width):
    half = keep.shape[0]
    return pl.pallas_call(
        functools.partial(attend_kernel, total_width),
        in_specs=[IN_SMEM] + [IN_VMEM] * 5,
        out_specs=IN_VMEM,
        out_shape=vmem((half, query_width), jnp.bfloat16),
        compiler_params=pltpu.CompilerParams(vmem_limit_bytes=LIMIT),
        cost_estimate=pl.CostEstimate(flops=900_000_000, bytes_accessed=10**6, transcendentals=0),
        name="attend",
    )(picks, keep, keep_sq, recv, kv, lens)


def output_kernel(place, picks, own_ref, recv_ref, active_ref, xa_ref, xb_ref, w_ref, *refs):
    out_refs, att_ref = refs[:-1], refs[-1]
    upper = place[0]
    shard = place[1]
    group = BLOCK // 2
    blocks = att_ref.shape[0] // BLOCK
    for block in range(blocks):
        here = pl.ds(pl.multiple_of(block * BLOCK + shard * group, group), group)
        there = pl.ds(pl.multiple_of(block * BLOCK + (1 - shard) * group, group), group)
        rows = pl.ds(block * group, group)
        att_ref[here, :] = own_ref[rows, :]
        att_ref[there, :] = recv_ref[rows, :]
    active = jnp.concatenate([active_ref[picks[block]] for block in range(blocks)], axis=0) > upper
    tile = 512
    width = out_refs[0].shape[1]
    for start in range(0, xa_ref.shape[1], tile):
        columns = slice(start, start + tile)
        branch = jnp.dot(att_ref[...], w_ref[:, columns], preferred_element_type=jnp.float32)
        state = jnp.where(upper == 0, xa_ref[:, columns], xb_ref[:, columns]).astype(jnp.float32)
        updated = jnp.where(active, state + branch, state).astype(jnp.bfloat16)
        out_refs[start // width][:, start % width : start % width + tile] = updated


def output(place, picks, own, recv, exits, xa, xb, w, parts):
    rows, features = xa.shape
    depth = w.shape[0]
    return pl.pallas_call(
        output_kernel,
        in_specs=[IN_SMEM, IN_SMEM] + [IN_VMEM] * 6,
        out_specs=[IN_VMEM] * parts,
        out_shape=[vmem((rows, features // parts), jnp.bfloat16)] * parts,
        scratch_shapes=[pltpu.VMEM((rows, depth), jnp.bfloat16)],
        compiler_params=pltpu.CompilerParams(vmem_limit_bytes=LIMIT),
        cost_estimate=pl.CostEstimate(
            flops=2 * rows * features * depth,
            bytes_accessed=2 * features * depth + 6 * rows * features,
            transcendentals=0,
        ),
        name="output",
    )(place, picks, own, recv, exits, xa, xb, w)


def paired_body(hidden, exit_layer, lengths, kv_cache, norm_gain, w_qkv, w_out):
    index = lax.axis_index("section")
    upper = index // 2
    shard = index % 2
    swap = [(i, i ^ 1) for i in range(4)]
    up = [(0, 2), (1, 3)]
    down = [(2, 0), (3, 1)]
    gain = norm_gain
    proj_weight = w_qkv[0]
    out_weight = w_out[0]
    features = proj_weight.shape[0]
    query_width = out_weight.shape[0]
    group = BLOCK // 2
    context = kv_cache.shape[2]
    tall = 2 * BLOCK
    count = MICRO // 2
    kv = kv_cache[0]
    own_lengths = lax.dynamic_index_in_dim(lengths.reshape(MICRO, 2, group), shard, 1, False)
    lens = jnp.repeat(own_lengths, context, axis=1).reshape(MICRO, group // 16, 16 * context)
    place = jnp.stack([upper, shard]).astype(jnp.int32)
    exits = exit_layer.reshape(MICRO, BLOCK, 1)

    def blocks_of(chunk):
        first = 4 * (chunk % 2) + chunk // 2
        return first, first + 2

    states = split(hidden[0], tall)
    moved = [lax.ppermute(piece, "section", down) for piece in states]
    arrived = []
    finals = []
    held_proj = None
    held_out = None
    for step in range(count + 2):
        lower_chunk = min(step, count - 1)
        upper_chunk = max(step - 2, 0)
        if step < 2:
            xa = xb = states[step]
        elif step < count:
            xa = moved[step - 2]
            xb = arrived[step - 2]
        else:
            xa = xb = arrived[step - 2]
        low = blocks_of(lower_chunk)
        high = blocks_of(upper_chunk)
        picks = jnp.where(upper == 0, jnp.array(low, jnp.int32), jnp.array(high, jnp.int32))
        if step == 0:
            keep, keep_sq, send = project(place, xa, xb, gain, proj_weight)
        elif step == 1:
            keep, keep_sq, send = project(place, xa, xb, gain, proj_weight)
        else:
            keep, keep_sq, send = project(place, xa, xb, gain, proj_weight)
        if step == 1:
            jobs.append((picks, xa, xb, keep, keep_sq, send))
        else:
            jobs = [(picks, xa, xb, keep, keep_sq, send)]
        if step == 0:
            continue
        for number, (picks, xa, xb, keep, keep_sq, send) in enumerate(jobs):
            at = step - len(jobs) + 1 + number
            received = lax.ppermute(send, "section", swap)
            own = attend(float(2 * features), picks, keep, keep_sq, received, kv, lens, query_width)
            other = lax.ppermute(own, "section", swap)
            if at < 2:
                (state,) = output(place, picks, own, other, exits, xa, xb, out_weight, 1)
                arrived.append(lax.ppermute(state, "section", up))
            elif at < count:
                state_low, state_high = output(place, picks, own, other, exits, xa, xb, out_weight, 2)
                state = jnp.concatenate([state_low, state_high], axis=1)
                arrived.append(lax.ppermute(state, "section", up))
            else:
                state_low, state_high = output(place, picks, own, other, exits, xa, xb, out_weight, 2)
            if at >= 2:
                settled = lax.ppermute(state_low, "section", down)
                finals.append(jnp.where(upper == 0, settled, state_high))
    pieces = [None] * MICRO
    for chunk in range(count):
        for place_in, block in enumerate(blocks_of(chunk)):
            pieces[block] = finals[chunk][place_in * BLOCK : (place_in + 1) * BLOCK]
    return jnp.concatenate(pieces, axis=0)


def solution(mesh):
    paired = mesh.shape["section"] == 4
    return jax.shard_map(
        paired_body if paired else body,
        mesh=mesh,
        in_specs=(
            P("section", "blk", None),
            P("blk"),
            P("blk"),
            P("section", "blk", None, None),
            P("section", None),
            P("section", None, None),
            P("section", None, None),
        ),
        out_specs=P("blk", "section"),
        check_vma=False,
    )
```

```python
import functools
import math

import jax
import jax.numpy as jnp
from jax import lax
from jax.experimental import pallas as pl
from jax.experimental.pallas import tpu as pltpu
from jax.sharding import PartitionSpec as P


BLOCK = 64
MICRO = 8


EPSILON = 1e-05
NEGATIVE = -1e30


def partner(value, axis, distance):
    return lax.ppermute(value, axis, [(i, i ^ 1 << distance) for i in range(lax.axis_size(axis))])


def shifted(value, axis, steps):
    count = lax.axis_size(axis)
    pairs = [(source, (source + steps) % count) for source in range(count)]
    return lax.ppermute(value, axis, pairs)


def body(hidden, exit_layer, lengths, kv_cache, norm_gain, w_qkv, w_out):
    devices = lax.axis_size("section")
    index = lax.axis_index("section")
    shards = max(2, devices // 4)
    cycle_size = devices // shards
    segment_bits = cycle_size.bit_length() - 1
    shard_bits = shards.bit_length() - 1
    segment_index = index // shards
    shard_index = index % shards
    own_blocks = hidden[0]
    gain_row = norm_gain[0].astype(jnp.float32)
    proj_weight = w_qkv[0]
    out_weight = w_out[0]
    cache_all = kv_cache[0]
    query_width = out_weight.shape[0]
    head_size = (proj_weight.shape[1] - query_width) // 2
    heads = query_width // head_size
    quarter = proj_weight.shape[0]
    total_width = quarter * shards
    group_rows = BLOCK // shards
    rounds = MICRO // cycle_size
    context = cache_all.shape[1]
    positions = jnp.arange(context, dtype=jnp.int32)
    blank_block = jnp.zeros((BLOCK, quarter), jnp.bfloat16)

    def advance(carry, microstep):
        incoming, arriving, records = carry
        micro_index = microstep - segment_index
        in_range = (micro_index >= 0) & (micro_index < MICRO)
        slot = jnp.clip(micro_index, 0, MICRO - 1)
        on_turn = microstep % cycle_size == 0
        local_slot = jnp.minimum(microstep // cycle_size, rounds - 1)
        own_block = lax.dynamic_slice_in_dim(own_blocks, local_slot * BLOCK, BLOCK, 0)
        exit_rows = lax.dynamic_slice_in_dim(exit_layer, slot * BLOCK, BLOCK)
        own_lengths = lax.dynamic_slice_in_dim(
            lengths, slot * BLOCK + shard_index * group_rows, group_rows
        )
        own_cache = lax.dynamic_slice_in_dim(cache_all, slot * group_rows, group_rows, 0)
        first_input = jnp.where(on_turn, own_block, arriving)
        entering = jnp.where(segment_index == 0, first_input, incoming)
        active = exit_rows > segment_index
        gate = in_range & (jnp.sum(active.astype(jnp.int32)) > 0)

        def local_partials():
            widened = entering.astype(jnp.float32)
            scaled = (widened * gain_row).astype(jnp.bfloat16)
            return (
                jnp.dot(scaled, proj_weight, preferred_element_type=jnp.float32),
                jnp.sum(widened * widened, axis=1),
            )

        def no_partials():
            return (
                jnp.zeros((BLOCK, proj_weight.shape[1]), jnp.float32),
                jnp.zeros((BLOCK,), jnp.float32),
            )

        partial_proj, partial_squares = lax.cond(gate, local_partials, no_partials)
        kept = (partial_proj, partial_squares)
        for level in range(shard_bits):
            bit = shard_bits - 1 - level
            upper = index >> bit & 1
            halves = tuple(
                (piece.reshape((2, piece.shape[0] // 2) + piece.shape[1:]) for piece in kept)
            )
            keep = tuple((jnp.where(upper == 1, half[1], half[0]) for half in halves))
            send = tuple((jnp.where(upper == 1, half[0], half[1]) for half in halves))
            received = partner(send, "section", bit)
            kept = tuple((first + second for first, second in zip(keep, received)))
        own_proj, own_squares = kept

        def local_attention():
            fitted = own_proj * lax.rsqrt(own_squares / total_width + EPSILON)[:, None]
            query = (fitted[:, :query_width] * (1.0 / math.sqrt(head_size))).astype(jnp.bfloat16)
            query = query.reshape(group_rows, heads, head_size)
            key_new = fitted[:, query_width : query_width + head_size].astype(jnp.bfloat16)
            value_new = fitted[:, query_width + head_size :].astype(jnp.bfloat16)
            scores = jnp.einsum(
                "rhd,rcd->rhc",
                query,
                own_cache[:, :, :head_size],
                preferred_element_type=jnp.float32,
            )
            own = jnp.einsum("rhd,rd->rh", query, key_new, preferred_element_type=jnp.float32)
            usable = (positions[None, :] < own_lengths[:, None])[:, None, :]
            scores = jnp.where(usable, scores, NEGATIVE)
            row_top = jnp.maximum(jnp.max(scores, axis=-1), own)
            raw = jnp.where(usable, jnp.exp(scores - row_top[:, :, None]), jnp.float32(0.0))
            raw_own = jnp.exp(own - row_top)
            total = jnp.sum(raw, axis=-1) + raw_own
            weights = (raw / total[:, :, None]).astype(jnp.bfloat16)
            own_weight = (raw_own / total).astype(jnp.bfloat16)
            attended = jnp.einsum(
                "rhc,rcd->rhd",
                weights,
                own_cache[:, :, head_size:],
                preferred_element_type=jnp.float32,
            )
            attended = (
                attended
                + own_weight.astype(jnp.float32)[:, :, None]
                * value_new.astype(jnp.float32)[:, None, :]
            )
            return attended.astype(jnp.bfloat16).reshape(group_rows, query_width)

        def no_attention():
            return jnp.zeros((group_rows, query_width), jnp.bfloat16)

        collected = lax.cond(gate, local_attention, no_attention)
        for level in range(shard_bits):
            bit = level
            other = partner(collected, "section", bit)
            upper = index >> bit & 1
            collected = jnp.where(
                upper == 1,
                jnp.concatenate([other, collected], 0),
                jnp.concatenate([collected, other], 0),
            )

        def local_update():
            branch_out = jnp.dot(collected, out_weight, preferred_element_type=jnp.float32)
            updated = (entering.astype(jnp.float32) + branch_out).astype(jnp.bfloat16)
            return jnp.where(active[:, None], updated, entering)

        def keep_state():
            return entering

        outgoing = lax.cond(gate, local_update, keep_state)
        leaving = in_range & (exit_rows == segment_index + 1)
        previous = lax.dynamic_slice_in_dim(records, slot * BLOCK, BLOCK, 0)
        records = lax.dynamic_update_slice_in_dim(
            records, jnp.where(leaving[:, None], outgoing, previous), slot * BLOCK, 0
        )
        relayed = jnp.where(on_turn & (segment_index > 0), own_block, arriving)
        incoming, arriving = shifted((outgoing, relayed), "section", shards)
        return ((incoming, arriving, records), None)

    start = (blank_block, blank_block, jnp.zeros((MICRO * BLOCK, quarter), jnp.bfloat16))
    carry, _ = lax.scan(advance, start, jnp.arange(MICRO + cycle_size - 1, dtype=jnp.int32))
    kept = carry[2]
    for level in range(segment_bits):
        bit = shard_bits + segment_bits - 1 - level
        upper = index >> bit & 1
        halves = kept.reshape(kept.shape[0], 2, kept.shape[1] // 2)
        keep = jnp.where(upper == 1, halves[:, 1], halves[:, 0])
        send = jnp.where(upper == 1, halves[:, 0], halves[:, 1])
        received = partner(send, "section", bit)
        kept = (keep.astype(jnp.float32) + received.astype(jnp.float32)).astype(jnp.bfloat16)
    return kept


CAPACITY = 40
LIMIT = 10 * 1024 * 1024
IN_VMEM = pl.BlockSpec(memory_space=pltpu.VMEM)
IN_SMEM = pl.BlockSpec(memory_space=pltpu.SMEM)
IN_HBM = pl.BlockSpec(memory_space=pltpu.HBM)


def call(kernel, inputs, in_specs, outs, out_specs=None, scratch=(), flops=10**8, **more):
    return pl.pallas_call(
        kernel,
        in_specs=in_specs,
        out_specs=[IN_VMEM] * len(outs) if out_specs is None else out_specs,
        out_shape=outs,
        scratch_shapes=scratch,
        compiler_params=pltpu.CompilerParams(vmem_limit_bytes=LIMIT),
        cost_estimate=pl.CostEstimate(flops=flops, bytes_accessed=10**6, transcendentals=0),
        **more,
    )(*inputs)


def seat():
    index = lax.axis_index("section")
    return index // 2, index % 2


def chunk_blocks(chunk):
    first = 4 * (chunk % 2) + chunk // 2
    return first, first + 2


def same_group(shape):
    half = BLOCK // 2
    first = lax.broadcasted_iota(jnp.int32, shape, 0)
    second = lax.broadcasted_iota(jnp.int32, shape, 1)
    return (first // half) % 2 == (second // half) % 2, first, second


def chunk_rows(values):
    lanes = lax.broadcasted_iota(jnp.int32, (1, 2 * BLOCK), 1)
    rows = []
    for chunk in range(4):
        upper_row = values[2 * (chunk % 2) : 2 * (chunk % 2) + 1]
        lower_row = values[2 * (chunk % 2) + 1 : 2 * (chunk % 2) + 2]
        if chunk < 2:
            rows.append(jnp.where(lanes < BLOCK, upper_row, pltpu.roll(lower_row, BLOCK, 1)))
        else:
            rows.append(jnp.where(lanes < BLOCK, pltpu.roll(upper_row, BLOCK, 1), lower_row))
    return jnp.concatenate(rows + rows, axis=0)


def exact_dot(a, b):
    return jnp.dot(
        a.astype(jnp.bfloat16), b.astype(jnp.bfloat16), preferred_element_type=jnp.float32
    )


def split_kernel(x_ref, *refs):
    outs, sem = refs[:-1], refs[-1]
    tall = outs[0].shape[0]
    copies = [
        pltpu.make_async_copy(x_ref.at[pl.ds(i * tall, tall)], out, sem.at[i])
        for i, out in enumerate(outs)
    ]
    for copy in copies:
        copy.start()
    for copy in copies:
        copy.wait()


def prepare_kernel(exit_ref, length_ref, order_ref, active_ref, limit_ref, fit_ref):
    upper, shard = seat()
    tall = 2 * BLOCK
    half = BLOCK // 2
    values = chunk_rows(exit_ref[...].astype(jnp.float32))
    deep = (values > 1).astype(jnp.float32)
    same, first, second = same_group((tall, tall))
    same = same.astype(jnp.float32)
    ahead = jnp.where(first <= second, same, 0.0)
    counts = exact_dot(deep, same)
    fit_ref[0] = (jnp.max(counts) <= float(CAPACITY)).astype(jnp.int32)
    rank = jnp.where(
        deep > 0, exact_dot(deep, ahead) - 1, counts + exact_dot(1 - deep, ahead) - 1
    )
    lanes = lax.broadcasted_iota(jnp.int32, rank.shape, 1)
    target = rank.astype(jnp.int32) + ((lanes // half) % 2) * BLOCK
    for chunk in range(4):
        order = first == target[chunk : chunk + 1]
        order_ref[chunk] = order.astype(jnp.float32).astype(jnp.bfloat16)
        natural = (first == second) & (values[chunk : chunk + 1] > 0)
        ranked = order & (deep[chunk : chunk + 1] > 0)
        chosen = jnp.where(
            upper == 0, natural.astype(jnp.float32), ranked.astype(jnp.float32)
        )
        column = jnp.sum(chosen, axis=1, keepdims=True)
        active_ref[chunk] = jnp.broadcast_to(column, (tall, 128))
    context = limit_ref.shape[2] // half
    lengths = length_ref[...].astype(jnp.float32)
    lengths = jnp.concatenate([lengths, lengths], axis=0)
    source = lax.broadcasted_iota(jnp.int32, (tall, limit_ref.shape[2]), 0)
    column = lax.broadcasted_iota(jnp.int32, (tall, limit_ref.shape[2]), 1)
    for parity in range(2):
        spread = source == parity * BLOCK + shard * half + column // context
        limit_ref[parity] = exact_dot(lengths, spread.astype(jnp.float32))


def framed(pieces, height):
    rows = []
    for piece in pieces:
        piece = piece.astype(jnp.float32)
        rows.append(piece)
        if piece.shape[0] < height:
            rows.append(jnp.zeros((height - piece.shape[0], piece.shape[1]), jnp.float32))
    return jnp.concatenate(rows, axis=0)


def own_rows(upper, shard, piece, rows):
    half = BLOCK // 2
    base = jnp.where(upper == 0, piece * BLOCK + shard * half, shard * BLOCK + piece * half)
    return pl.ds(pl.multiple_of(base, half), rows)


def project_kernel(roles, load, *refs):
    refs = list(refs)
    x_ref = refs.pop(0) if roles != "upper" else None
    a_ref = refs.pop(0) if roles != "lower" else None
    gain_ref, w_ref = refs.pop(0), refs.pop(0)
    if load == "second":
        other_ref, cache_ref = refs.pop(0), refs.pop(0)
    keep_ref, keep_sq_ref, send_ref = refs.pop(0), refs.pop(0), refs.pop(0)
    if load:
        held_ref, sem = refs.pop(0), refs.pop()
    if load == "second":
        held_cache_ref = refs.pop(0)
    xs_ref, acc_ref, sq_ref = refs
    upper, shard = seat()
    features = w_ref.shape[0]
    pieces = 4
    depth = features // pieces
    copies = []
    if load == "first":
        copies = [
            pltpu.make_async_copy(
                w_ref.at[pl.ds(i * depth, depth)], held_ref.at[pl.ds(i * depth, depth)], sem.at[i]
            )
            for i in range(pieces)
        ]
    elif load == "second":
        copies = [
            pltpu.make_async_copy(other_ref, held_ref, sem.at[0]),
            pltpu.make_async_copy(cache_ref, held_cache_ref, sem.at[1]),
        ]
    for copy in copies:
        copy.start()

    def scale(read):
        squares = None
        for i in range(pieces):
            columns = slice(i * depth, (i + 1) * depth)
            x = read(columns)
            for lane in range(0, depth, 128):
                part = x[:, lane : lane + 128]
                squares = part * part if squares is None else squares + part * part
            xs_ref[:, columns] = (x * gain_ref[:, columns].astype(jnp.float32)).astype(jnp.bfloat16)
        sq_ref[...] = squares

    if roles != "upper":
        @pl.when(upper == 0)
        def _():
            scale(lambda columns: x_ref[:, columns].astype(jnp.float32))

    if roles != "lower":
        @pl.when(upper != 0)
        def _():
            scale(lambda columns: framed([a_ref[g, :, columns] for g in range(2)], BLOCK))

    def multiply():
        if load == "first":
            for i in range(pieces):
                columns = slice(i * depth, (i + 1) * depth)
                copies[i].wait()
                product = jnp.dot(
                    xs_ref[:, columns], held_ref[columns, :], preferred_element_type=jnp.float32
                )
                if i == 0:
                    acc_ref[...] = product
                else:
                    acc_ref[...] += product
        else:
            acc_ref[...] = jnp.dot(xs_ref[...], w_ref[...], preferred_element_type=jnp.float32)
        half = BLOCK // 2
        width = keep_ref.shape[1]
        for piece in range(2):
            here = own_rows(upper, shard, piece, half)
            there = own_rows(upper, 1 - shard, piece, half)
            rows = pl.ds(piece * half, half)
            keep_ref[rows, :] = acc_ref[here, :]
            send_ref[rows, :width] = acc_ref[there, :].astype(jnp.bfloat16)
            own = jnp.sum(sq_ref[here, :], axis=1, keepdims=True)
            keep_sq_ref[rows, :] = jnp.broadcast_to(own, (half, 128))
            other = jnp.broadcast_to(jnp.sum(sq_ref[there, :], axis=1, keepdims=True), (half, 128))
            high = other.astype(jnp.bfloat16).astype(jnp.float32)
            lanes = lax.broadcasted_iota(jnp.int32, (half, 128), 1)
            send_ref[rows, width:] = jnp.where(lanes < 64, high, other - high).astype(jnp.bfloat16)

    if load == "first":
        multiply()
    elif roles == "both":
        multiply()
    else:
        pl.when((upper == 0) if roles == "lower" else (upper != 0))(multiply)
    if load == "second":
        for copy in copies:
            copy.wait()


def project(roles, x, a, gain, w, load=None, other=None, cache=None):
    features, width = w.shape
    tall = 2 * BLOCK
    inputs = [x] * (roles != "upper") + [a] * (roles != "lower") + [gain, w]
    specs = [IN_VMEM] * len(inputs)
    outs = [
        pltpu.VMEM((BLOCK, width), jnp.float32),
        pltpu.VMEM((BLOCK, 128), jnp.float32),
        pltpu.VMEM((BLOCK, width + 128), jnp.bfloat16),
    ]
    scratch = [
        pltpu.VMEM((tall, features), jnp.bfloat16),
        pltpu.VMEM((tall, width), jnp.float32),
        pltpu.VMEM((tall, 128), jnp.float32),
    ]
    if load == "first":
        specs[-1] = IN_HBM
        outs.append(pltpu.VMEM(w.shape, w.dtype))
        scratch.append(pltpu.SemaphoreType.DMA((4,)))
    elif load == "second":
        inputs += [other, cache]
        specs += [IN_HBM, IN_HBM]
        outs += [pltpu.VMEM(other.shape, other.dtype), pltpu.VMEM(cache.shape, cache.dtype)]
        scratch.append(pltpu.SemaphoreType.DMA((2,)))
    return call(
        functools.partial(project_kernel, roles, load), inputs, specs, outs, scratch=scratch,
        flops=2 * tall * features * width,
    )


def by_role(roles, upper, lower_part, upper_part):
    if roles == "both":
        pl.when(upper == 0)(lower_part)
        pl.when(upper != 0)(upper_part)
    elif roles == "lower":
        lower_part()
    else:
        upper_part()


def attend_kernel(roles, low, high, total_width, keep_ref, keep_sq_ref, recv_ref, kv_ref, limit_ref, order_ref, out_ref,
                  fit_ref, wide_ref, att_ref, spread_ref):
    upper, shard = seat()
    if roles != "both":
        pl.when((upper == 0) if roles == "lower" else (upper != 0))(
            functools.partial(
                attend_rows, roles, low if roles == "lower" else high, total_width, upper, shard, keep_ref, keep_sq_ref,
                recv_ref, kv_ref, limit_ref, order_ref, out_ref, fit_ref, wide_ref, att_ref, spread_ref,
            )
        )
    else:
        attend_rows(
            roles, jnp.where(upper == 0, low, high), total_width, upper, shard, keep_ref, keep_sq_ref,
            recv_ref, kv_ref, limit_ref, order_ref, out_ref, fit_ref, wide_ref, att_ref, spread_ref,
        )


def attend_rows(roles, chunk, total_width, upper, shard, keep_ref, keep_sq_ref, recv_ref, kv_ref, limit_ref, order_ref,
                out_ref, fit_ref, wide_ref, att_ref, spread_ref):
    width = keep_ref.shape[1]
    query_width = out_ref.shape[1]
    context = kv_ref.shape[1]
    head_size = kv_ref.shape[2] // 2
    heads = query_width // head_size
    half = BLOCK // 2
    tokens = 16
    columns = tokens * context
    other = recv_ref[:, width:].astype(jnp.float32)
    squares = keep_sq_ref[:, :1] + other[:, :1] + other[:, 64:65]
    factor = lax.rsqrt(squares / total_width + EPSILON)
    fitted = (keep_ref[...] + recv_ref[:, :width].astype(jnp.float32)) * factor
    scale = 1.0 / math.sqrt(head_size)
    rounded = jnp.concatenate(
        [
            (fitted[:, :query_width] * scale).astype(jnp.bfloat16),
            fitted[:, query_width:].astype(jnp.bfloat16),
        ],
        axis=1,
    )

    def natural():
        fit_ref[...] = rounded

    def restored():
        own_order = order_ref[chunk, pl.ds(pl.multiple_of(shard * BLOCK, BLOCK), BLOCK), :]
        wide_ref[...] = lax.dot_general(
            own_order, rounded, (((0,), (0,)), ((), ())), preferred_element_type=jnp.float32
        )
        for piece in range(2):
            rows = pl.ds(pl.multiple_of(piece * BLOCK + shard * half, half), half)
            fit_ref[piece * half : (piece + 1) * half, :] = wide_ref[rows, :].astype(jnp.bfloat16)

    by_role(roles, upper, natural, restored)
    row = lax.broadcasted_iota(jnp.int32, (heads * tokens, columns), 0)
    column = lax.broadcasted_iota(jnp.int32, (heads * tokens, columns), 1)
    same = (row % tokens) == (column // context)
    position = (lax.broadcasted_iota(jnp.int32, (1, columns), 1) % context).astype(jnp.float32)
    parity = chunk // 2
    first_row = 2 * (chunk % 2)
    pieces = [(block, part) for block in range(2) for part in range(half // tokens)]
    queries, scores, owns, masks, tops, raws, raw_owns, totals = [], [], [], [], [], [], [], []

    def cache_rows(block, part):
        first = (2 * (first_row + block) + parity) * half + part * tokens
        return pl.ds(pl.multiple_of(first, tokens), tokens)

    for block, part in pieces:
        base = block * half + part * tokens
        rows = slice(base, base + tokens)
        queries.append(
            jnp.concatenate(
                [fit_ref[rows, h * head_size : (h + 1) * head_size] for h in range(heads)], axis=0
            )
        )
    for i, (block, part) in enumerate(pieces):
        rows = slice(block * half + part * tokens, block * half + (part + 1) * tokens)
        keys = kv_ref[cache_rows(block, part), :, :head_size].reshape(columns, head_size)
        scores.append(
            lax.dot_general(
                queries[i], keys, (((1,), (1,)), ((), ())), preferred_element_type=jnp.float32
            )
        )
        key_new = fit_ref[rows, query_width : query_width + head_size].astype(jnp.float32)
        key_new = jnp.concatenate([key_new] * heads, axis=0)
        owns.append(jnp.sum(queries[i].astype(jnp.float32) * key_new, axis=1, keepdims=True))
    for i, (block, part) in enumerate(pieces):
        limit = limit_ref[parity, pl.ds(first_row + block, 1), part * columns : (part + 1) * columns]
        masks.append(same & (position < limit))
        scores[i] = jnp.where(masks[i], scores[i], NEGATIVE)
        tops.append(jnp.maximum(jnp.max(scores[i], axis=1, keepdims=True), owns[i]))
    for i in range(len(pieces)):
        raws.append(jnp.where(masks[i], jnp.exp(scores[i] - tops[i]), 0.0))
        raw_owns.append(jnp.exp(owns[i] - tops[i]))
        totals.append(jnp.sum(raws[i], axis=1, keepdims=True) + raw_owns[i])
    for i, (block, part) in enumerate(pieces):
        rows = slice(block * half + part * tokens, block * half + (part + 1) * tokens)
        values = kv_ref[cache_rows(block, part), :, head_size:].reshape(columns, head_size)
        weights = (raws[i] / totals[i]).astype(jnp.bfloat16)
        own_weight = (raw_owns[i] / totals[i]).astype(jnp.bfloat16).astype(jnp.float32)
        value_new = fit_ref[rows, query_width + head_size :].astype(jnp.float32)
        value_new = jnp.concatenate([value_new] * heads, axis=0)
        attended = jnp.dot(weights, values, preferred_element_type=jnp.float32)
        attended = (attended + own_weight * value_new).astype(jnp.bfloat16)
        for h in range(heads):
            att_ref[rows, h * head_size : (h + 1) * head_size] = attended[
                h * tokens : (h + 1) * tokens
            ]

    def kept():
        out_ref[...] = att_ref[...]

    def ranked():
        spread_ref[...] = jnp.zeros_like(spread_ref)
        for piece in range(2):
            rows = pl.ds(pl.multiple_of(piece * BLOCK + shard * half, half), half)
            spread_ref[rows, :] = att_ref[piece * half : (piece + 1) * half, :]
        own_order = order_ref[chunk, pl.ds(pl.multiple_of(shard * BLOCK, BLOCK), BLOCK), :]
        out_ref[...] = jnp.dot(
            own_order, spread_ref[...], preferred_element_type=jnp.float32
        ).astype(jnp.bfloat16)

    by_role(roles, upper, kept, ranked)


def attend(roles, low, high, total_width, keep, keep_sq, recv, kv, limits, order, query_width):
    width = keep.shape[1]
    tall = 2 * BLOCK
    return call(
        functools.partial(attend_kernel, roles, low, high, total_width),
        [keep, keep_sq, recv, kv, limits, order], [IN_VMEM] * 6,
        [pltpu.VMEM((BLOCK, query_width), jnp.bfloat16)],
        scratch=[
            pltpu.VMEM((BLOCK, width), jnp.bfloat16),
            pltpu.VMEM((tall, width), jnp.float32),
            pltpu.VMEM((BLOCK, query_width), jnp.bfloat16),
            pltpu.VMEM((tall, query_width), jnp.bfloat16),
        ],
        flops=900_000_000,
    )[0]


def output_kernel(roles, low, high, *refs):
    refs = list(refs)
    own_ref, recv_ref, active_ref, order_ref = refs[:4]
    refs = refs[4:]
    x_ref = refs.pop(0) if roles != "upper" else None
    a_ref = refs.pop(0) if roles != "lower" else None
    w_ref = refs.pop(0)
    if roles != "upper":
        up_ref, high_rest_ref, low_rest_ref = refs[:3]
        refs = refs[3:]
    if roles != "lower":
        low_ref, high_ref = refs[:2]
        refs = refs[2:]
    (att_ref,) = refs
    upper, shard = seat()
    chunk = jnp.where(upper == 0, low, high)
    half = BLOCK // 2
    tile = 512
    features = w_ref.shape[1]
    middle = features // 2

    def gather():
        for piece in range(2):
            rows = pl.ds(piece * half, half)
            att_ref[own_rows(upper, shard, piece, half), :] = own_ref[rows, :]
            att_ref[own_rows(upper, 1 - shard, piece, half), :] = recv_ref[rows, :]

    def updated(columns, state):
        branch = jnp.dot(att_ref[...], w_ref[:, columns], preferred_element_type=jnp.float32)
        active = active_ref[chunk][:, :1] > 0
        return jnp.where(active, state + branch, state)

    if roles != "upper":
        @pl.when(upper == 0)
        def _():
            gather()
            order = order_ref[low]

            def each(i, carry):
                inner = pl.ds(pl.multiple_of(i * tile, tile), tile)
                for side, rest_ref in enumerate((low_rest_ref, high_rest_ref)):
                    columns = pl.ds(pl.multiple_of(i * tile + side * middle, tile), tile)
                    state = updated(columns, x_ref[:, columns].astype(jnp.float32))
                    sorted_rows = jnp.dot(
                        order, state.astype(jnp.bfloat16), preferred_element_type=jnp.float32
                    )
                    for g in range(2):
                        top = g * BLOCK
                        up_ref[g, :, columns] = sorted_rows[top : top + CAPACITY].astype(jnp.bfloat16)
                        rest_ref[g, :, inner] = sorted_rows[top + CAPACITY : top + BLOCK].astype(jnp.bfloat16)
                return carry

            lax.fori_loop(0, middle // tile, each, 0)

    if roles != "lower":
        @pl.when(upper != 0)
        def _():
            gather()

            def each(i, carry):
                inner = pl.ds(pl.multiple_of(i * tile, tile), tile)
                for side, half_ref in enumerate((low_ref, high_ref)):
                    columns = pl.ds(pl.multiple_of(i * tile + side * middle, tile), tile)
                    state = updated(columns, framed([a_ref[g, :, columns] for g in range(2)], BLOCK))
                    for g in range(2):
                        top = g * BLOCK
                        half_ref[g, :, inner] = state[top : top + CAPACITY].astype(jnp.bfloat16)
                return carry

            lax.fori_loop(0, middle // tile, each, 0)


def output(roles, low, high, own, recv, active, order, x, a, w):
    depth, features = w.shape
    middle = features // 2
    inputs = [own, recv, active, order] + [x] * (roles != "upper") + [a] * (roles != "lower") + [w]
    rest = BLOCK - CAPACITY
    outs = []
    if roles != "upper":
        outs += [
            pltpu.VMEM((2, CAPACITY, features), jnp.bfloat16),
            pltpu.VMEM((2, rest, middle), jnp.bfloat16),
            pltpu.VMEM((2, rest, middle), jnp.bfloat16),
        ]
    if roles != "lower":
        outs += [pltpu.VMEM((2, CAPACITY, middle), jnp.bfloat16)] * 2
    return call(
        functools.partial(output_kernel, roles, low, high), inputs, [IN_VMEM] * len(inputs), outs,
        scratch=[pltpu.VMEM((2 * BLOCK, depth), jnp.bfloat16)],
        flops=4 * BLOCK * features * depth,
    )


def settle_kernel(chunk, fresh, *refs):
    order_ref, d_ref, own_rest_ref, own_high_ref, recv_rest_ref = refs[:5]
    refs = refs[5:] if fresh else refs[6:]
    out_ref, rows_ref, sem = refs
    upper, _ = seat()
    order = order_ref[chunk]
    tile = 512

    def place(first, rest):
        for start in range(0, rows_ref.shape[1], tile):
            columns = slice(start, start + tile)
            pieces = []
            for g in range(2):
                pieces += [
                    first[g, :, columns].astype(jnp.float32),
                    rest[g, :, columns].astype(jnp.float32),
                ]
            frame = jnp.concatenate(pieces, axis=0).astype(jnp.bfloat16)
            rows_ref[:, columns] = lax.dot_general(
                order, frame, (((0,), (0,)), ((), ())), preferred_element_type=jnp.float32
            ).astype(jnp.bfloat16)

    @pl.when(upper == 0)
    def _():
        place(d_ref, own_rest_ref)

    @pl.when(upper != 0)
    def _():
        place(own_high_ref, recv_rest_ref)

    copies = [
        pltpu.make_async_copy(
            rows_ref.at[pl.ds(i * BLOCK, BLOCK)], out_ref.at[pl.ds(block * BLOCK, BLOCK)], sem.at[i]
        )
        for i, block in enumerate(chunk_blocks(chunk))
    ]
    for copy in copies:
        copy.start()
    for copy in copies:
        copy.wait()


def settle(chunk, order, d, own_rest, own_high, recv_rest, out):
    width = d.shape[2]
    fresh = out is None
    inputs = [order, d, own_rest, own_high, recv_rest] + ([] if fresh else [out])
    return call(
        functools.partial(settle_kernel, chunk, fresh), inputs,
        [IN_VMEM] * 5 + ([] if fresh else [IN_HBM]),
        [jax.ShapeDtypeStruct((MICRO * BLOCK, width), jnp.bfloat16)], [IN_HBM],
        scratch=[pltpu.VMEM((2 * BLOCK, width), jnp.bfloat16), pltpu.SemaphoreType.DMA((2,))],
        flops=4 * BLOCK * 2 * BLOCK * width,
        input_output_aliases={} if fresh else {5: 0},
    )[0]


def compact(hidden, exit_layer, lengths, kv_cache, norm_gain, w_qkv, w_out):
    swap = [(i, i ^ 1) for i in range(4)]
    up = [(0, 2), (1, 3)]
    down = [(2, 0), (3, 1)]
    features = w_qkv.shape[1]
    query_width = w_out.shape[1]
    context = kv_cache.shape[2]
    tall = 2 * BLOCK
    count = 4
    lag = 3
    exits = exit_layer.reshape(4, tall)
    length_rows = lengths.reshape(4, tall)
    total_width = float(2 * features)

    def send(value, pairs):
        return lax.ppermute(value, "section", pairs)

    states = call(
        split_kernel, [hidden[0]], [IN_HBM],
        [pltpu.VMEM((tall, features), jnp.bfloat16)] * 2,
        scratch=[pltpu.SemaphoreType.DMA((2,))],
    )
    moved = [send(states[i], down) for i in range(2)]
    order, active, limits, fits = call(
        prepare_kernel, [exits, length_rows], [IN_VMEM] * 2,
        [
            pltpu.VMEM((4, tall, tall), jnp.bfloat16),
            pltpu.VMEM((4, tall, 128), jnp.float32),
            pltpu.VMEM((2, 8, BLOCK // 2 * context), jnp.float32),
            jax.ShapeDtypeStruct((1,), jnp.int32),
        ],
        [IN_VMEM] * 3 + [IN_SMEM],
    )
    arrived, low_rests, high_rests, settled, own_highs = [], [], [], [], []
    for step in range(count + lag):
        low, high = min(step, count - 1), max(step - lag, 0)
        roles = "lower" if step < lag else "both" if step < count else "upper"
        x = states[step] if step < 2 else moved[step - 2] if step < count else None
        a = arrived[step - lag] if step >= lag else None
        if step == 0:
            keep, keep_sq, partial, held_proj = project(
                roles, x, a, norm_gain, w_qkv[0], load="first"
            )
        elif step == 1:
            keep, keep_sq, partial, held_out, held_cache = project(
                roles, x, a, norm_gain, held_proj, "second", w_out[0], kv_cache[0]
            )
        else:
            keep, keep_sq, partial = project(roles, x, a, norm_gain, held_proj)
        if step == 0:
            waiting = (keep, keep_sq, partial, x, a, roles, low, high)
            continue
        jobs = [(keep, keep_sq, partial, x, a, roles, low, high)]
        if step == 1:
            jobs = [waiting] + jobs
        for keep, keep_sq, partial, x, a, roles, low, high in jobs:
            received = send(partial, swap)
            own = attend(roles, low, high, total_width, keep, keep_sq, received, held_cache, limits, order, query_width)
            other = send(own, swap)
            results = output(roles, low, high, own, other, active, order, x, a, held_out)
            if roles != "upper":
                arrived.append(send(results[0], up))
                high_rests.append(send(results[1], up))
                low_rests.append(results[2])
            if roles != "lower":
                settled.append(send(results[-2], down))
                own_highs.append(results[-1])
    out = None
    for chunk in range(count):
        out = settle(
            chunk, order, settled[chunk], low_rests[chunk], own_highs[chunk], high_rests[chunk], out
        )
    return out, fits


def paired_body(hidden, exit_layer, lengths, kv_cache, norm_gain, w_qkv, w_out):
    arguments = (hidden, exit_layer, lengths, kv_cache, norm_gain, w_qkv, w_out)
    out, fits = compact(*arguments)
    return lax.cond(fits[0] > 0, lambda out, *rest: out, lambda out, *rest: body(*rest), out, *arguments)


def solution(mesh):
    paired = mesh.shape["section"] == 4
    return jax.shard_map(
        paired_body if paired else body,
        mesh=mesh,
        in_specs=(
            P("section", "blk", None),
            P("blk"),
            P("blk"),
            P("section", "blk", None, None),
            P("section", None),
            P("section", None, None),
            P("section", None, None),
        ),
        out_specs=P("blk", "section"),
        check_vma=False,
    )
```

```python
import functools
import math

import jax
import jax.numpy as jnp
from jax import lax
from jax.experimental import pallas as pl
from jax.experimental.pallas import tpu as pltpu
from jax.sharding import PartitionSpec as P


BLOCK = 64
MICRO = 8


EPSILON = 1e-05
NEGATIVE = -1e30


def partner(value, axis, distance):
    return lax.ppermute(value, axis, [(i, i ^ 1 << distance) for i in range(lax.axis_size(axis))])


def shifted(value, axis, steps):
    count = lax.axis_size(axis)
    pairs = [(source, (source + steps) % count) for source in range(count)]
    return lax.ppermute(value, axis, pairs)


def body(hidden, exit_layer, lengths, kv_cache, norm_gain, w_qkv, w_out):
    devices = lax.axis_size("section")
    index = lax.axis_index("section")
    shards = max(2, devices // 4)
    cycle_size = devices // shards
    segment_bits = cycle_size.bit_length() - 1
    shard_bits = shards.bit_length() - 1
    segment_index = index // shards
    shard_index = index % shards
    own_blocks = hidden[0]
    gain_row = norm_gain[0].astype(jnp.float32)
    proj_weight = w_qkv[0]
    out_weight = w_out[0]
    cache_all = kv_cache[0]
    query_width = out_weight.shape[0]
    head_size = (proj_weight.shape[1] - query_width) // 2
    heads = query_width // head_size
    quarter = proj_weight.shape[0]
    total_width = quarter * shards
    group_rows = BLOCK // shards
    rounds = MICRO // cycle_size
    context = cache_all.shape[1]
    positions = jnp.arange(context, dtype=jnp.int32)
    blank_block = jnp.zeros((BLOCK, quarter), jnp.bfloat16)

    def advance(carry, microstep):
        incoming, arriving, records = carry
        micro_index = microstep - segment_index
        in_range = (micro_index >= 0) & (micro_index < MICRO)
        slot = jnp.clip(micro_index, 0, MICRO - 1)
        on_turn = microstep % cycle_size == 0
        local_slot = jnp.minimum(microstep // cycle_size, rounds - 1)
        own_block = lax.dynamic_slice_in_dim(own_blocks, local_slot * BLOCK, BLOCK, 0)
        exit_rows = lax.dynamic_slice_in_dim(exit_layer, slot * BLOCK, BLOCK)
        own_lengths = lax.dynamic_slice_in_dim(
            lengths, slot * BLOCK + shard_index * group_rows, group_rows
        )
        own_cache = lax.dynamic_slice_in_dim(cache_all, slot * group_rows, group_rows, 0)
        first_input = jnp.where(on_turn, own_block, arriving)
        entering = jnp.where(segment_index == 0, first_input, incoming)
        active = exit_rows > segment_index
        gate = in_range & (jnp.sum(active.astype(jnp.int32)) > 0)

        def local_partials():
            widened = entering.astype(jnp.float32)
            scaled = (widened * gain_row).astype(jnp.bfloat16)
            return (
                jnp.dot(scaled, proj_weight, preferred_element_type=jnp.float32),
                jnp.sum(widened * widened, axis=1),
            )

        def no_partials():
            return (
                jnp.zeros((BLOCK, proj_weight.shape[1]), jnp.float32),
                jnp.zeros((BLOCK,), jnp.float32),
            )

        partial_proj, partial_squares = lax.cond(gate, local_partials, no_partials)
        kept = (partial_proj, partial_squares)
        for level in range(shard_bits):
            bit = shard_bits - 1 - level
            upper = index >> bit & 1
            halves = tuple(
                (piece.reshape((2, piece.shape[0] // 2) + piece.shape[1:]) for piece in kept)
            )
            keep = tuple((jnp.where(upper == 1, half[1], half[0]) for half in halves))
            send = tuple((jnp.where(upper == 1, half[0], half[1]) for half in halves))
            received = partner(send, "section", bit)
            kept = tuple((first + second for first, second in zip(keep, received)))
        own_proj, own_squares = kept

        def local_attention():
            fitted = own_proj * lax.rsqrt(own_squares / total_width + EPSILON)[:, None]
            query = (fitted[:, :query_width] * (1.0 / math.sqrt(head_size))).astype(jnp.bfloat16)
            query = query.reshape(group_rows, heads, head_size)
            key_new = fitted[:, query_width : query_width + head_size].astype(jnp.bfloat16)
            value_new = fitted[:, query_width + head_size :].astype(jnp.bfloat16)
            scores = jnp.einsum(
                "rhd,rcd->rhc",
                query,
                own_cache[:, :, :head_size],
                preferred_element_type=jnp.float32,
            )
            own = jnp.einsum("rhd,rd->rh", query, key_new, preferred_element_type=jnp.float32)
            usable = (positions[None, :] < own_lengths[:, None])[:, None, :]
            scores = jnp.where(usable, scores, NEGATIVE)
            row_top = jnp.maximum(jnp.max(scores, axis=-1), own)
            raw = jnp.where(usable, jnp.exp(scores - row_top[:, :, None]), jnp.float32(0.0))
            raw_own = jnp.exp(own - row_top)
            total = jnp.sum(raw, axis=-1) + raw_own
            weights = (raw / total[:, :, None]).astype(jnp.bfloat16)
            own_weight = (raw_own / total).astype(jnp.bfloat16)
            attended = jnp.einsum(
                "rhc,rcd->rhd",
                weights,
                own_cache[:, :, head_size:],
                preferred_element_type=jnp.float32,
            )
            attended = (
                attended
                + own_weight.astype(jnp.float32)[:, :, None]
                * value_new.astype(jnp.float32)[:, None, :]
            )
            return attended.astype(jnp.bfloat16).reshape(group_rows, query_width)

        def no_attention():
            return jnp.zeros((group_rows, query_width), jnp.bfloat16)

        collected = lax.cond(gate, local_attention, no_attention)
        for level in range(shard_bits):
            bit = level
            other = partner(collected, "section", bit)
            upper = index >> bit & 1
            collected = jnp.where(
                upper == 1,
                jnp.concatenate([other, collected], 0),
                jnp.concatenate([collected, other], 0),
            )

        def local_update():
            branch_out = jnp.dot(collected, out_weight, preferred_element_type=jnp.float32)
            updated = (entering.astype(jnp.float32) + branch_out).astype(jnp.bfloat16)
            return jnp.where(active[:, None], updated, entering)

        def keep_state():
            return entering

        outgoing = lax.cond(gate, local_update, keep_state)
        leaving = in_range & (exit_rows == segment_index + 1)
        previous = lax.dynamic_slice_in_dim(records, slot * BLOCK, BLOCK, 0)
        records = lax.dynamic_update_slice_in_dim(
            records, jnp.where(leaving[:, None], outgoing, previous), slot * BLOCK, 0
        )
        relayed = jnp.where(on_turn & (segment_index > 0), own_block, arriving)
        incoming, arriving = shifted((outgoing, relayed), "section", shards)
        return ((incoming, arriving, records), None)

    start = (blank_block, blank_block, jnp.zeros((MICRO * BLOCK, quarter), jnp.bfloat16))
    carry, _ = lax.scan(advance, start, jnp.arange(MICRO + cycle_size - 1, dtype=jnp.int32))
    kept = carry[2]
    for level in range(segment_bits):
        bit = shard_bits + segment_bits - 1 - level
        upper = index >> bit & 1
        halves = kept.reshape(kept.shape[0], 2, kept.shape[1] // 2)
        keep = jnp.where(upper == 1, halves[:, 1], halves[:, 0])
        send = jnp.where(upper == 1, halves[:, 0], halves[:, 1])
        received = partner(send, "section", bit)
        kept = (keep.astype(jnp.float32) + received.astype(jnp.float32)).astype(jnp.bfloat16)
    return kept


UNROLL = 1
AHEAD = 4
LIMIT = 6 * 1024 * 1024
CHUNKS = ((0, 2), (4, 6), (1, 3), (5, 7))
IN_VMEM = pl.BlockSpec(memory_space=pltpu.VMEM)
IN_SMEM = pl.BlockSpec(memory_space=pltpu.SMEM)
IN_HBM = pl.BlockSpec(memory_space=pltpu.HBM)


def call(kernel, inputs, in_specs, outs, out_specs=None, scratch=(), flops=10**8, **more):
    return pl.pallas_call(
        kernel,
        in_specs=in_specs,
        out_specs=[IN_VMEM] * len(outs) if out_specs is None else out_specs,
        out_shape=outs,
        scratch_shapes=scratch,
        compiler_params=pltpu.CompilerParams(vmem_limit_bytes=LIMIT),
        cost_estimate=pl.CostEstimate(flops=flops, bytes_accessed=10**6, transcendentals=0),
        **more,
    )(*inputs)


def seat():
    index = lax.axis_index("section")
    return index // 2, index % 2


def on_layer(layer, body_fn):
    upper, _ = seat()
    pl.when(upper == layer)(body_fn)


def exact_dot(a, b):
    return jnp.dot(
        a.astype(jnp.bfloat16), b.astype(jnp.bfloat16), preferred_element_type=jnp.float32
    )


def kept_rows(chunk):
    return len(CHUNKS[chunk]) * BLOCK // 2


def arrange_kernel(x_ref, order_ref, cache_ref, *refs):
    next_ref, held_cache_ref, outs, rows_ref, sem = refs[0], refs[1], refs[2:-2], refs[-2], refs[-1]
    tall = next_ref.shape[0]
    second = pltpu.make_async_copy(x_ref.at[pl.ds(tall, tall)], next_ref, sem.at[0])
    second.start()
    cache = pltpu.make_async_copy(cache_ref, held_cache_ref, sem.at[2])
    cache.start()
    tile = 512

    def select(chunk, source_ref, deep_ref, rest_ref):
        kept = deep_ref.shape[0]

        def each(i, carry):
            columns = pl.ds(pl.multiple_of(i * tile, tile), tile)
            rows = jnp.dot(
                order_ref[chunk], source_ref[:, columns], preferred_element_type=jnp.float32
            ).astype(jnp.bfloat16)
            deep_ref[:, columns] = rows[:kept]
            rest_ref[:, columns] = rows[kept:]
            return carry

        lax.fori_loop(0, x_ref.shape[1] // tile, each, 0)

    def upper():
        first = pltpu.make_async_copy(x_ref.at[pl.ds(0, tall)], rows_ref, sem.at[1])
        first.start()
        first.wait()
        select(2, rows_ref, outs[0], outs[2])

    on_layer(1, upper)
    second.wait()
    on_layer(1, functools.partial(select, 3, next_ref, outs[1], outs[3]))
    cache.wait()


def arrange(x, order, cache):
    tall, features = 2 * BLOCK, x.shape[1]
    return call(
        arrange_kernel, [x, order, cache], [IN_HBM, IN_VMEM, IN_HBM],
        [pltpu.VMEM((tall, features), x.dtype), pltpu.VMEM(cache.shape, cache.dtype)]
        + [pltpu.VMEM((BLOCK, features), x.dtype)] * 4,
        scratch=[pltpu.VMEM((tall, features), x.dtype), pltpu.SemaphoreType.DMA((3,))],
    )


def chunk_rows(values):
    lanes = lax.broadcasted_iota(jnp.int32, (1, 2 * BLOCK), 1)
    rows = []
    for blocks in CHUNKS:
        halves = []
        for side, block in enumerate(blocks):
            row = values[block // 2 : block // 2 + 1]
            halves.append(row if block % 2 == side else pltpu.roll(row, BLOCK, 1))
        if len(halves) == 1:
            halves.append(jnp.full_like(halves[0], -1.0))
        rows.append(jnp.where(lanes < BLOCK, halves[0], halves[1]))
    while len(rows) < 8:
        rows.append(jnp.full_like(rows[0], -1.0))
    return jnp.concatenate(rows, axis=0)


def prepare_kernel(exit_ref, length_ref, order_ref, restore_ref, active_ref, limit_ref, excess_ref):
    upper, shard = seat()
    tall = 2 * BLOCK
    half = BLOCK // 2
    values = chunk_rows(exit_ref[...].astype(jnp.float32))
    deep = (values > 1).astype(jnp.float32)
    rest = ((values >= 0) & (values <= 1)).astype(jnp.float32)
    first = lax.broadcasted_iota(jnp.int32, (tall, tall), 0)
    second = lax.broadcasted_iota(jnp.int32, (tall, tall), 1)
    ahead = (first <= second).astype(jnp.float32)
    counts = jnp.sum(deep, axis=1, keepdims=True)
    excess = jnp.int32(0)
    rank = jnp.where(deep > 0, exact_dot(deep, ahead) - 1, counts + exact_dot(rest, ahead) - 1)
    rank = jnp.where(values >= 0, rank, -1.0).astype(jnp.int32)
    for chunk in range(len(CHUNKS)):
        over = jnp.max(counts[chunk : chunk + 1]) > float(kept_rows(chunk))
        excess = jnp.maximum(excess, over.astype(jnp.int32))
        target = rank[chunk : chunk + 1]
        order = first == target
        order_ref[chunk] = order.astype(jnp.float32).astype(jnp.bfloat16)
        column = jnp.sum(
            jnp.where(first == second, target, 0).astype(jnp.float32), axis=1, keepdims=True
        )
        restore = column.astype(jnp.int32) == second
        restore_ref[chunk] = restore.astype(jnp.float32).astype(jnp.bfloat16)
        natural = (first == second) & (values[chunk : chunk + 1] > 0)
        ranked = order & (deep[chunk : chunk + 1] > 0)
        chosen = jnp.where(upper == 0, natural.astype(jnp.float32), ranked.astype(jnp.float32))
        active_ref[chunk] = jnp.broadcast_to(jnp.sum(chosen, axis=1, keepdims=True), (tall, 128))
    excess_ref[0] = excess
    context = limit_ref.shape[2] // half
    lengths = length_ref[...].astype(jnp.float32)
    lengths = jnp.concatenate([lengths, lengths], axis=0)
    source = lax.broadcasted_iota(jnp.int32, (tall, limit_ref.shape[2]), 0)
    column = lax.broadcasted_iota(jnp.int32, (tall, limit_ref.shape[2]), 1)
    for parity in range(2):
        spread = source == parity * BLOCK + shard * half + column // context
        limit_ref[parity] = exact_dot(lengths, spread.astype(jnp.float32))


def prepare(exits, lengths, context):
    tall = 2 * BLOCK
    count = len(CHUNKS)
    return call(
        prepare_kernel, [exits, lengths], [IN_VMEM] * 2,
        [
            pltpu.VMEM((count, tall, tall), jnp.bfloat16),
            pltpu.VMEM((count, tall, tall), jnp.bfloat16),
            pltpu.VMEM((count, tall, 128), jnp.float32),
            pltpu.VMEM((2, 8, BLOCK // 2 * context), jnp.float32),
            jax.ShapeDtypeStruct((1,), jnp.int32),
        ],
        [IN_VMEM] * 4 + [IN_SMEM],
    )


def own_rows(shard, piece):
    half = BLOCK // 2
    return pl.ds(pl.multiple_of(piece * BLOCK + shard * half, half), half)


def project_kernel(jobs, load, *refs):
    refs = list(refs)
    x_refs = [refs.pop(0) for _ in jobs]
    restore_ref = refs.pop(0) if any(kind != "all" for _, _, kind in jobs) else None
    gain_ref, w_ref = refs.pop(0), refs.pop(0)
    if load == "second":
        other_ref = refs.pop(0)
    keep_ref, keep_sq_ref, send_ref = refs.pop(0), refs.pop(0), refs.pop(0)
    if load:
        held_ref, sem = refs.pop(0), refs.pop()
    if load == "first":
        first_ref = refs.pop(0)
        first_rows = pltpu.make_async_copy(x_refs[0].at[pl.ds(0, first_ref.shape[0])], first_ref, sem.at[8])
        first_rows.start()
        x_refs = [first_ref]
    acc_ref, sq_ref = refs
    _, shard = seat()
    features = w_ref.shape[0]
    pieces = 8 if load == "first" else 2
    depth = features // pieces

    def fetch(i):
        rows = pl.ds(pl.multiple_of(i * depth, depth), depth)
        return pltpu.make_async_copy(w_ref.at[rows], held_ref.at[rows], sem.at[i])

    copies = []
    if load == "first":
        for i in range(AHEAD):
            fetch(i).start()
    elif load == "second":
        copies = [pltpu.make_async_copy(other_ref, held_ref, sem.at[0])]
    for copy in copies:
        copy.start()

    def multiply(layer, chunk, kind, x_ref):
        tall = len(CHUNKS[chunk]) * BLOCK

        def each(i, carry):
            columns = pl.ds(pl.multiple_of(i * depth, depth), depth)
            if kind != "all":
                base = tall // 2 if kind == "rest" else 0
                restore = restore_ref[chunk][:tall, base : base + tall // 2]
                x = jnp.dot(restore, x_ref[:, columns], preferred_element_type=jnp.float32)
            else:
                x = x_ref[:, columns].astype(jnp.float32)
            squares = None
            for lane in range(0, depth, 128):
                part = x[:, lane : lane + 128]
                squares = part * part if squares is None else squares + part * part
            scaled = (x * gain_ref[:, columns].astype(jnp.float32)).astype(jnp.bfloat16)
            if load == "first":
                fetch(i).wait()

                @pl.when(i + AHEAD < pieces)
                def _():
                    fetch(i + AHEAD).start()

                weight = held_ref[columns, :]
            else:
                weight = w_ref[columns, :]
            product = jnp.dot(scaled, weight, preferred_element_type=jnp.float32)
            acc_ref[:tall, :] += product
            sq_ref[:tall, :] += squares
            return carry

        acc_ref[:tall, :] = jnp.zeros((tall, acc_ref.shape[1]), jnp.float32)
        sq_ref[:tall, :] = jnp.zeros((tall, sq_ref.shape[1]), jnp.float32)
        lax.fori_loop(0, pieces, each, 0)
        half = BLOCK // 2
        width = keep_ref.shape[1]
        for piece in range(tall // BLOCK):
            here = own_rows(shard, piece)
            there = own_rows(1 - shard, piece)
            rows = pl.ds(piece * half, half)
            keep_ref[rows, :] = acc_ref[here, :]
            send_ref[rows, :width] = acc_ref[there, :].astype(jnp.bfloat16)
            own = jnp.sum(sq_ref[here, :], axis=1, keepdims=True)
            keep_sq_ref[rows, :] = jnp.broadcast_to(own, (half, 128))
            other = jnp.broadcast_to(jnp.sum(sq_ref[there, :], axis=1, keepdims=True), (half, 128))
            high = other.astype(jnp.bfloat16).astype(jnp.float32)
            lanes = lax.broadcasted_iota(jnp.int32, (half, 128), 1)
            send_ref[rows, width:] = jnp.where(lanes < 64, high, other - high).astype(jnp.bfloat16)

    if load == "first":
        first_rows.wait()
    for job, x_ref in zip(jobs, x_refs):
        if load == "first":
            multiply(*job, x_ref)
        else:
            on_layer(job[0], functools.partial(multiply, *job, x_ref))
    if load == "second":
        for copy in copies:
            copy.wait()


def widest(jobs):
    return max(len(CHUNKS[chunk]) for _, chunk, _ in jobs) * BLOCK


def project(jobs, xs, restore, gain, w, load=None, other=None):
    features, width = w.shape
    tall = widest(jobs)
    own = tall // 2
    pooled = any(kind != "all" for _, _, kind in jobs)
    inputs = list(xs) + [restore] * pooled + [gain, w]
    specs = [IN_VMEM] * len(inputs)
    outs = [
        pltpu.VMEM((own, width), jnp.float32),
        pltpu.VMEM((own, 128), jnp.float32),
        pltpu.VMEM((own, width + 128), jnp.bfloat16),
    ]
    scratch = [
        pltpu.VMEM((tall, width), jnp.float32),
        pltpu.VMEM((tall, 128), jnp.float32),
    ]
    if load == "first":
        specs[0] = specs[-1] = IN_HBM
        outs += [pltpu.VMEM(w.shape, w.dtype), pltpu.VMEM((tall, features), jnp.bfloat16)]
        scratch.append(pltpu.SemaphoreType.DMA((9,)))
    elif load == "second":
        inputs.append(other)
        specs.append(IN_HBM)
        outs.append(pltpu.VMEM(other.shape, other.dtype))
        scratch.append(pltpu.SemaphoreType.DMA((1,)))
    return call(
        functools.partial(project_kernel, jobs, load), inputs, specs, outs, scratch=scratch,
        flops=2 * tall * features * width,
    )


def attend_kernel(jobs, total_width, *refs):
    for layer, chunk, _ in jobs:
        on_layer(layer, functools.partial(attend_rows, chunk, total_width, *refs))


def attend_rows(chunk, total_width, keep_ref, keep_sq_ref, recv_ref, kv_ref, limit_ref, out_ref, fit_ref):
    width = keep_ref.shape[1]
    query_width = out_ref.shape[1]
    context = kv_ref.shape[1]
    head_size = kv_ref.shape[2] // 2
    heads = query_width // head_size
    half = BLOCK // 2
    tokens = 16
    columns = tokens * context
    count = len(CHUNKS[chunk]) * half
    other = recv_ref[:count, width:].astype(jnp.float32)
    squares = keep_sq_ref[:count, :1] + other[:, :1] + other[:, 64:65]
    factor = lax.rsqrt(squares / total_width + EPSILON)
    fitted = (keep_ref[:count, :] + recv_ref[:count, :width].astype(jnp.float32)) * factor
    scale = 1.0 / math.sqrt(head_size)
    fit_ref[:count, :query_width] = (fitted[:, :query_width] * scale).astype(jnp.bfloat16)
    fit_ref[:count, query_width:] = fitted[:, query_width:].astype(jnp.bfloat16)
    row = lax.broadcasted_iota(jnp.int32, (heads * tokens, columns), 0)
    column = lax.broadcasted_iota(jnp.int32, (heads * tokens, columns), 1)
    same = (row % tokens) == (column // context)
    position = (lax.broadcasted_iota(jnp.int32, (1, columns), 1) % context).astype(jnp.float32)
    pieces = [
        (place * half + part * tokens, block, part)
        for place, block in enumerate(CHUNKS[chunk])
        for part in range(half // tokens)
    ]
    queries, scores, owns, masks, tops, raws, raw_owns, totals = [], [], [], [], [], [], [], []
    for base, block, part in pieces:
        rows = slice(base, base + tokens)
        queries.append(
            jnp.concatenate(
                [fit_ref[rows, h * head_size : (h + 1) * head_size] for h in range(heads)], axis=0
            )
        )
    for i, (base, block, part) in enumerate(pieces):
        cached = slice(block * half + part * tokens, block * half + (part + 1) * tokens)
        keys = kv_ref[cached, :, :head_size].reshape(columns, head_size)
        scores.append(
            lax.dot_general(
                queries[i], keys, (((1,), (1,)), ((), ())), preferred_element_type=jnp.float32
            )
        )
        key_new = fit_ref[base : base + tokens, query_width : query_width + head_size]
        key_new = jnp.concatenate([key_new.astype(jnp.float32)] * heads, axis=0)
        owns.append(jnp.sum(queries[i].astype(jnp.float32) * key_new, axis=1, keepdims=True))
    for i, (base, block, part) in enumerate(pieces):
        line = block // 2
        limit = limit_ref[block % 2, line : line + 1, part * columns : (part + 1) * columns]
        masks.append(same & (position < limit))
        scores[i] = jnp.where(masks[i], scores[i], NEGATIVE)
        tops.append(jnp.maximum(jnp.max(scores[i], axis=1, keepdims=True), owns[i]))
    for i in range(len(pieces)):
        raws.append(jnp.where(masks[i], jnp.exp(scores[i] - tops[i]), 0.0))
        raw_owns.append(jnp.exp(owns[i] - tops[i]))
        totals.append(jnp.sum(raws[i], axis=1, keepdims=True) + raw_owns[i])
    for i, (base, block, part) in enumerate(pieces):
        rows = slice(base, base + tokens)
        cached = slice(block * half + part * tokens, block * half + (part + 1) * tokens)
        values = kv_ref[cached, :, head_size:].reshape(columns, head_size)
        weights = (raws[i] / totals[i]).astype(jnp.bfloat16)
        own_weight = (raw_owns[i] / totals[i]).astype(jnp.bfloat16).astype(jnp.float32)
        value_new = fit_ref[rows, query_width + head_size :].astype(jnp.float32)
        value_new = jnp.concatenate([value_new] * heads, axis=0)
        attended = jnp.dot(weights, values, preferred_element_type=jnp.float32)
        attended = (attended + own_weight * value_new).astype(jnp.bfloat16)
        for h in range(heads):
            out_ref[rows, h * head_size : (h + 1) * head_size] = attended[
                h * tokens : (h + 1) * tokens
            ]


def attend(jobs, total_width, keep, keep_sq, recv, kv, limits, query_width):
    own = keep.shape[0]
    return call(
        functools.partial(attend_kernel, jobs, total_width),
        [keep, keep_sq, recv, kv, limits], [IN_VMEM] * 5,
        [pltpu.VMEM((own, query_width), jnp.bfloat16)],
        scratch=[pltpu.VMEM((own, keep.shape[1]), jnp.bfloat16)],
        flops=900_000_000,
    )[0]


def output_kernel(jobs, own_ref, recv_ref, active_ref, order_ref, *refs):
    refs = list(refs)
    x_refs = [refs.pop(0) for _ in jobs]
    carry_ref = refs.pop(0) if jobs[-1][0] else None
    w_ref, att_ref = refs.pop(0), refs.pop()
    _, shard = seat()
    half = BLOCK // 2
    tile = 512
    middle = w_ref.shape[1] // 2

    def gather(tall):
        for piece in range(tall // BLOCK):
            rows = pl.ds(piece * half, half)
            att_ref[own_rows(shard, piece), :] = own_ref[rows, :]
            att_ref[own_rows(1 - shard, piece), :] = recv_ref[rows, :]

    def updated(chunk, x_ref, rows, columns, base=0):
        state = x_ref[:, columns].astype(jnp.float32)
        branch = jnp.dot(rows, w_ref[:, columns], preferred_element_type=jnp.float32)[: state.shape[0]]
        active = active_ref[chunk][base : base + state.shape[0], :1] > 0
        return jnp.where(active, state + branch, state).astype(jnp.bfloat16)

    def lower(chunk, x_ref, up_ref, high_rest_ref, low_rest_ref):
        tall = x_ref.shape[0]
        kept = tall // 2
        gather(tall)
        order = order_ref[chunk][:tall, :tall]

        def each(i, carry):
            inner = pl.ds(pl.multiple_of(i * tile, tile), tile)
            for side, rest_ref in enumerate((low_rest_ref, high_rest_ref)):
                columns = pl.ds(pl.multiple_of(i * tile + side * middle, tile), tile)
                state = updated(chunk, x_ref, att_ref[:tall, :], columns)
                ordered = jnp.dot(order, state, preferred_element_type=jnp.float32)
                up_ref[:, columns] = ordered[:kept].astype(jnp.bfloat16)
                rest_ref[:, inner] = ordered[kept:].astype(jnp.bfloat16)
            return carry

        lax.fori_loop(0, middle // tile, each, 0, unroll=UNROLL)

    def pooled(chunk, kind, x_ref, *outs):
        kept = x_ref.shape[0]
        tall = 2 * kept
        base = kept if kind == "rest" else 0
        gather(tall)
        rows = jnp.dot(
            order_ref[chunk][base : base + kept, :tall], att_ref[:tall, :], preferred_element_type=jnp.float32
        )
        att_ref[:kept, :] = rows.astype(jnp.bfloat16)

        def each(i, carry):
            inner = pl.ds(pl.multiple_of(i * tile, tile), tile)
            for side in range(2):
                columns = pl.ds(pl.multiple_of(i * tile + side * middle, tile), tile)
                state = updated(chunk, x_ref, att_ref[:tall, :], columns, base)
                if len(outs) == 1:
                    outs[0][:, columns] = state
                else:
                    outs[side][:, inner] = state
            return carry

        lax.fori_loop(0, middle // tile, each, 0, unroll=UNROLL)

    for (layer, chunk, kind), x_ref in zip(jobs, x_refs):
        outs = [refs.pop(0) for _ in range(len(result_shapes(layer, chunk, kind, 2 * middle)))]
        if kind == "all":
            on_layer(layer, functools.partial(lower, chunk, x_ref, *outs))
        else:
            on_layer(layer, functools.partial(pooled, chunk, kind, x_ref, *outs))
        if layer:
            swap_ref = outs[0]

            def ship():
                swap_ref[...] = carry_ref[...]

            on_layer(0, ship)


def result_shapes(layer, chunk, kind, features):
    kept = kept_rows(chunk)
    whole = pltpu.VMEM((kept, features), jnp.bfloat16)
    part = pltpu.VMEM((kept, features // 2), jnp.bfloat16)
    if layer or kind == "rest":
        return [part, part]
    return [whole, part, part] if kind == "all" else [whole]


def output(jobs, own, recv, active, order, xs, carry, w):
    depth, features = w.shape
    outs = []
    for job in jobs:
        outs += result_shapes(*job, features)
    inputs = [own, recv, active, order, *xs] + [carry] * jobs[-1][0] + [w]
    return call(
        functools.partial(output_kernel, jobs), inputs, [IN_VMEM] * len(inputs), outs,
        scratch=[pltpu.VMEM((widest(jobs), depth), jnp.bfloat16)],
        flops=2 * widest(jobs) * features * depth,
    )


def settle_rows(chunk, restore_ref, refs, rows_ref):
    received_ref, own_rest_ref, own_high_ref = refs
    tile = 512
    tall = rows_ref.shape[0]

    def place(first, rest):
        restore = restore_ref[chunk][:tall, :tall]

        def each(i, carry):
            columns = pl.ds(pl.multiple_of(i * tile, tile), tile)
            rows = jnp.concatenate([first[:, columns], rest[:, columns]], axis=0)
            rows_ref[:, columns] = jnp.dot(
                restore, rows, preferred_element_type=jnp.float32
            ).astype(jnp.bfloat16)
            return carry

        lax.fori_loop(0, rows_ref.shape[1] // tile, each, 0)

    on_layer(0, functools.partial(place, received_ref, own_rest_ref))
    on_layer(1, functools.partial(place, own_high_ref, received_ref))


def settle_kernel(jobs, restore_ref, *refs):
    outs = refs[3 * len(jobs) :]
    for i, chunk in enumerate(jobs):
        settle_rows(chunk, restore_ref, refs[3 * i : 3 * i + 3], outs[i])


def settled_shape(chunk, width):
    return pltpu.VMEM((len(CHUNKS[chunk]) * BLOCK, width), jnp.bfloat16)


def settle(jobs, restore, operands):
    width = operands[0].shape[1]
    inputs = [restore, *operands]
    return call(
        functools.partial(settle_kernel, jobs), inputs, [IN_VMEM] * len(inputs),
        [settled_shape(chunk, width) for chunk in jobs],
    )


def finish_kernel(jobs, restore_ref, *refs):
    count = len(CHUNKS) - len(jobs)
    ready, refs = refs[:count], refs[count:]
    operands, refs = refs[: 3 * len(jobs)], refs[3 * len(jobs) :]
    out_ref, rows_refs, sem = refs[0], refs[1:-1], refs[-1]
    started = []

    def put(chunk, rows_ref):
        for i, block in enumerate(CHUNKS[chunk]):
            copy = pltpu.make_async_copy(
                rows_ref.at[pl.ds(i * BLOCK, BLOCK)], out_ref.at[pl.ds(block * BLOCK, BLOCK)], sem.at[block]
            )
            copy.start()
            started.append(copy)

    for chunk in range(count):
        put(chunk, ready[chunk])
    for i, chunk in enumerate(jobs):
        settle_rows(chunk, restore_ref, operands[3 * i : 3 * i + 3], rows_refs[i])
        put(chunk, rows_refs[i])
    for copy in started:
        copy.wait()


def finish(jobs, restore, ready, operands, tokens):
    width = operands[0].shape[1]
    inputs = [restore, *ready, *operands]
    return call(
        functools.partial(finish_kernel, jobs), inputs, [IN_VMEM] * len(inputs),
        [pltpu.HBM((tokens, width), jnp.bfloat16)], [IN_HBM],
        scratch=[settled_shape(chunk, width) for chunk in jobs] + [pltpu.SemaphoreType.DMA((MICRO,))],
    )[0]


def hand_over_kernel(x_ref, out_ref):
    out_ref[...] = x_ref[...]


def hand_over(x):
    return call(hand_over_kernel, [x], [IN_VMEM], [jax.ShapeDtypeStruct(x.shape, x.dtype)])[0]


LAG = 3
SETTLES = ((0, 1), (2,), (3,))


def compact(hidden, exit_layer, lengths, kv_cache, norm_gain, w_qkv, w_out):
    swap = [(i, i ^ 1) for i in range(4)]
    up = [(0, 2), (1, 3)]
    down = [(2, 0), (3, 1)]
    across = [(i, i ^ 2) for i in range(4)]
    query_width = w_out.shape[1]
    total_width = float(2 * w_qkv.shape[1])
    count = len(CHUNKS)

    def send(value, pairs):
        return lax.ppermute(value, "section", pairs)

    order, restore, active, limits, excess = prepare(
        exit_layer.reshape(4, 2 * BLOCK), lengths.reshape(4, 2 * BLOCK), kv_cache.shape[2]
    )
    second, held_cache, *pooled = arrange(hidden[0], order, kv_cache[0])
    moved = [send(value, down) for value in pooled]
    entries = [hidden[0], second] + moved
    kinds = [(0, "all"), (1, "all"), (2, "deep"), (3, "deep"), (2, "rest"), (3, "rest")]
    arrived, settled, own_highs = [], [], []
    high_rests, low_rests = {}, {}
    queue = []

    def exchange(at, jobs, xs, keep, keep_sq, partial):
        received = send(partial, swap)
        own = attend(jobs, total_width, keep, keep_sq, received, held_cache, limits, query_width)
        other = send(own, swap)
        carry = high_rests[at - LAG] if at >= LAG else None
        results = list(output(jobs, own, other, active, order, xs, carry, held_out))
        for layer, chunk, kind in jobs:
            if layer:
                settled.append(send(results.pop(0), across))
                own_highs.append(results.pop(0))
                continue
            if kind != "rest":
                arrived.append(send(results.pop(0), up))
            if kind == "all":
                high_rests[chunk] = results.pop(0)
                low_rests[chunk] = results.pop(0)
            elif kind == "rest":
                low_rests[chunk] = results.pop(0)
                high_rests[chunk] = results.pop(0)

    for at in range(count + LAG):
        jobs, xs = [], []
        if at < len(kinds):
            jobs.append((0, *kinds[at]))
            xs.append(entries[at])
        if at >= LAG:
            jobs.append((1, at - LAG, "deep"))
            xs.append(arrived[at - LAG])
        if at == 0:
            *result, held_proj, first = project(jobs, xs, restore, norm_gain, w_qkv[0], "first")
            xs = [first]
        elif at == 1:
            *result, held_out = project(jobs, xs, restore, norm_gain, held_proj, "second", w_out[0])
        else:
            result = project(jobs, xs, restore, norm_gain, held_proj)
        queue.append((at, jobs, xs, *result))
        if at:
            for item in queue:
                exchange(*item)
            queue = []

    def settle_operands(chunks):
        return [
            value for c in chunks for value in (settled[c], low_rests[c], own_highs[c])
        ]

    ready = []
    for i, chunks in enumerate(SETTLES):
        if i + 1 < len(SETTLES):
            ready += settle(chunks, restore, settle_operands(chunks))
        else:
            out = finish(chunks, restore, ready, settle_operands(chunks), MICRO * BLOCK)
    arguments = (hidden, exit_layer, lengths, kv_cache, norm_gain, w_qkv, w_out)
    return lax.cond(excess[0] > 0, lambda out, *rest: hand_over(body(*rest)), lambda out, *rest: out, out, *arguments)


def solution(mesh):
    paired = mesh.shape["section"] == 4
    return jax.shard_map(
        compact if paired else body,
        mesh=mesh,
        in_specs=(
            P("section", "blk", None),
            P("blk"),
            P("blk"),
            P("section", "blk", None, None),
            P("section", None),
            P("section", None, None),
            P("section", None, None),
        ),
        out_specs=P("blk", "section"),
        check_vma=False,
    )
```

```python
import functools
import math

import jax
import jax.numpy as jnp
from jax import lax
from jax.experimental import pallas as pl
from jax.experimental.pallas import tpu as pltpu
from jax.sharding import PartitionSpec as P


BLOCK = 64
MICRO = 8


EPSILON = 1e-05
NEGATIVE = -1e30


def partner(value, axis, distance):
    return lax.ppermute(value, axis, [(i, i ^ 1 << distance) for i in range(lax.axis_size(axis))])


def shifted(value, axis, steps):
    count = lax.axis_size(axis)
    pairs = [(source, (source + steps) % count) for source in range(count)]
    return lax.ppermute(value, axis, pairs)


def body(hidden, exit_layer, lengths, kv_cache, norm_gain, w_qkv, w_out):
    devices = lax.axis_size("section")
    index = lax.axis_index("section")
    shards = max(2, devices // 4)
    cycle_size = devices // shards
    segment_bits = cycle_size.bit_length() - 1
    shard_bits = shards.bit_length() - 1
    segment_index = index // shards
    shard_index = index % shards
    own_blocks = hidden[0]
    gain_row = norm_gain[0].astype(jnp.float32)
    proj_weight = w_qkv[0]
    out_weight = w_out[0]
    cache_all = kv_cache[0]
    query_width = out_weight.shape[0]
    head_size = (proj_weight.shape[1] - query_width) // 2
    heads = query_width // head_size
    quarter = proj_weight.shape[0]
    total_width = quarter * shards
    group_rows = BLOCK // shards
    rounds = MICRO // cycle_size
    context = cache_all.shape[1]
    positions = jnp.arange(context, dtype=jnp.int32)
    blank_block = jnp.zeros((BLOCK, quarter), jnp.bfloat16)

    def advance(carry, microstep):
        incoming, arriving, records = carry
        micro_index = microstep - segment_index
        in_range = (micro_index >= 0) & (micro_index < MICRO)
        slot = jnp.clip(micro_index, 0, MICRO - 1)
        on_turn = microstep % cycle_size == 0
        local_slot = jnp.minimum(microstep // cycle_size, rounds - 1)
        own_block = lax.dynamic_slice_in_dim(own_blocks, local_slot * BLOCK, BLOCK, 0)
        exit_rows = lax.dynamic_slice_in_dim(exit_layer, slot * BLOCK, BLOCK)
        own_lengths = lax.dynamic_slice_in_dim(
            lengths, slot * BLOCK + shard_index * group_rows, group_rows
        )
        own_cache = lax.dynamic_slice_in_dim(cache_all, slot * group_rows, group_rows, 0)
        first_input = jnp.where(on_turn, own_block, arriving)
        entering = jnp.where(segment_index == 0, first_input, incoming)
        active = exit_rows > segment_index
        gate = in_range & (jnp.sum(active.astype(jnp.int32)) > 0)

        def local_partials():
            widened = entering.astype(jnp.float32)
            scaled = (widened * gain_row).astype(jnp.bfloat16)
            return (
                jnp.dot(scaled, proj_weight, preferred_element_type=jnp.float32),
                jnp.sum(widened * widened, axis=1),
            )

        def no_partials():
            return (
                jnp.zeros((BLOCK, proj_weight.shape[1]), jnp.float32),
                jnp.zeros((BLOCK,), jnp.float32),
            )

        partial_proj, partial_squares = lax.cond(gate, local_partials, no_partials)
        kept = (partial_proj, partial_squares)
        for level in range(shard_bits):
            bit = shard_bits - 1 - level
            upper = index >> bit & 1
            halves = tuple(
                (piece.reshape((2, piece.shape[0] // 2) + piece.shape[1:]) for piece in kept)
            )
            keep = tuple((jnp.where(upper == 1, half[1], half[0]) for half in halves))
            send = tuple((jnp.where(upper == 1, half[0], half[1]) for half in halves))
            received = partner(send, "section", bit)
            kept = tuple((first + second for first, second in zip(keep, received)))
        own_proj, own_squares = kept

        def local_attention():
            fitted = own_proj * lax.rsqrt(own_squares / total_width + EPSILON)[:, None]
            query = (fitted[:, :query_width] * (1.0 / math.sqrt(head_size))).astype(jnp.bfloat16)
            query = query.reshape(group_rows, heads, head_size)
            key_new = fitted[:, query_width : query_width + head_size].astype(jnp.bfloat16)
            value_new = fitted[:, query_width + head_size :].astype(jnp.bfloat16)
            scores = jnp.einsum(
                "rhd,rcd->rhc",
                query,
                own_cache[:, :, :head_size],
                preferred_element_type=jnp.float32,
            )
            own = jnp.einsum("rhd,rd->rh", query, key_new, preferred_element_type=jnp.float32)
            usable = (positions[None, :] < own_lengths[:, None])[:, None, :]
            scores = jnp.where(usable, scores, NEGATIVE)
            row_top = jnp.maximum(jnp.max(scores, axis=-1), own)
            raw = jnp.where(usable, jnp.exp(scores - row_top[:, :, None]), jnp.float32(0.0))
            raw_own = jnp.exp(own - row_top)
            total = jnp.sum(raw, axis=-1) + raw_own
            weights = (raw / total[:, :, None]).astype(jnp.bfloat16)
            own_weight = (raw_own / total).astype(jnp.bfloat16)
            attended = jnp.einsum(
                "rhc,rcd->rhd",
                weights,
                own_cache[:, :, head_size:],
                preferred_element_type=jnp.float32,
            )
            attended = (
                attended
                + own_weight.astype(jnp.float32)[:, :, None]
                * value_new.astype(jnp.float32)[:, None, :]
            )
            return attended.astype(jnp.bfloat16).reshape(group_rows, query_width)

        def no_attention():
            return jnp.zeros((group_rows, query_width), jnp.bfloat16)

        collected = lax.cond(gate, local_attention, no_attention)
        for level in range(shard_bits):
            bit = level
            other = partner(collected, "section", bit)
            upper = index >> bit & 1
            collected = jnp.where(
                upper == 1,
                jnp.concatenate([other, collected], 0),
                jnp.concatenate([collected, other], 0),
            )

        def local_update():
            branch_out = jnp.dot(collected, out_weight, preferred_element_type=jnp.float32)
            updated = (entering.astype(jnp.float32) + branch_out).astype(jnp.bfloat16)
            return jnp.where(active[:, None], updated, entering)

        def keep_state():
            return entering

        outgoing = lax.cond(gate, local_update, keep_state)
        leaving = in_range & (exit_rows == segment_index + 1)
        previous = lax.dynamic_slice_in_dim(records, slot * BLOCK, BLOCK, 0)
        records = lax.dynamic_update_slice_in_dim(
            records, jnp.where(leaving[:, None], outgoing, previous), slot * BLOCK, 0
        )
        relayed = jnp.where(on_turn & (segment_index > 0), own_block, arriving)
        incoming, arriving = shifted((outgoing, relayed), "section", shards)
        return ((incoming, arriving, records), None)

    start = (blank_block, blank_block, jnp.zeros((MICRO * BLOCK, quarter), jnp.bfloat16))
    carry, _ = lax.scan(advance, start, jnp.arange(MICRO + cycle_size - 1, dtype=jnp.int32))
    kept = carry[2]
    for level in range(segment_bits):
        bit = shard_bits + segment_bits - 1 - level
        upper = index >> bit & 1
        halves = kept.reshape(kept.shape[0], 2, kept.shape[1] // 2)
        keep = jnp.where(upper == 1, halves[:, 1], halves[:, 0])
        send = jnp.where(upper == 1, halves[:, 0], halves[:, 1])
        received = partner(send, "section", bit)
        kept = (keep.astype(jnp.float32) + received.astype(jnp.float32)).astype(jnp.bfloat16)
    return kept


LIMIT = 6 * 1024 * 1024
CHUNKS = ((0, 2), (4, 6), (1, 3), (5, 7))
IN_VMEM = pl.BlockSpec(memory_space=pltpu.VMEM)
IN_SMEM = pl.BlockSpec(memory_space=pltpu.SMEM)
IN_HBM = pl.BlockSpec(memory_space=pltpu.HBM)


def call(kernel, inputs, in_specs, outs, out_specs=None, scratch=(), flops=10**8, **more):
    return pl.pallas_call(
        kernel,
        in_specs=in_specs,
        out_specs=[IN_VMEM] * len(outs) if out_specs is None else out_specs,
        out_shape=outs,
        scratch_shapes=scratch,
        compiler_params=pltpu.CompilerParams(vmem_limit_bytes=LIMIT),
        cost_estimate=pl.CostEstimate(flops=flops, bytes_accessed=10**6, transcendentals=0),
        **more,
    )(*inputs)


def seat():
    index = lax.axis_index("section")
    return index // 2, index % 2


def on_layer(layer, body_fn):
    upper, _ = seat()
    pl.when(upper == layer)(body_fn)


def exact_dot(a, b):
    return jnp.dot(
        a.astype(jnp.bfloat16), b.astype(jnp.bfloat16), preferred_element_type=jnp.float32
    )


def kept_rows(chunk):
    return len(CHUNKS[chunk]) * BLOCK // 2


def arrange_kernel(x_ref, order_ref, cache_ref, *refs):
    next_ref, held_cache_ref, outs, rows_ref, sem = refs[0], refs[1], refs[2:-2], refs[-2], refs[-1]
    tall = next_ref.shape[0]
    second = pltpu.make_async_copy(x_ref.at[pl.ds(tall, tall)], next_ref, sem.at[0])
    second.start()
    cache = pltpu.make_async_copy(cache_ref, held_cache_ref, sem.at[2])
    cache.start()
    tile = 512

    def select(chunk, source_ref, deep_ref, rest_ref):
        kept = deep_ref.shape[0]

        def each(i, carry):
            columns = pl.ds(pl.multiple_of(i * tile, tile), tile)
            rows = jnp.dot(
                order_ref[chunk], source_ref[:, columns], preferred_element_type=jnp.float32
            ).astype(jnp.bfloat16)
            deep_ref[:, columns] = rows[:kept]
            rest_ref[:, columns] = rows[kept:]
            return carry

        lax.fori_loop(0, x_ref.shape[1] // tile, each, 0)

    def upper():
        first = pltpu.make_async_copy(x_ref.at[pl.ds(0, tall)], rows_ref, sem.at[1])
        first.start()
        first.wait()
        select(2, rows_ref, outs[0], outs[2])

    on_layer(1, upper)
    second.wait()
    on_layer(1, functools.partial(select, 3, next_ref, outs[1], outs[3]))
    cache.wait()


def arrange(x, order, cache):
    tall, features = 2 * BLOCK, x.shape[1]
    return call(
        arrange_kernel, [x, order, cache], [IN_HBM, IN_VMEM, IN_HBM],
        [pltpu.VMEM((tall, features), x.dtype), pltpu.VMEM(cache.shape, cache.dtype)]
        + [pltpu.VMEM((BLOCK, features), x.dtype)] * 4,
        scratch=[pltpu.VMEM((tall, features), x.dtype), pltpu.SemaphoreType.DMA((3,))],
    )


def chunk_rows(values):
    lanes = lax.broadcasted_iota(jnp.int32, (1, 2 * BLOCK), 1)
    rows = []
    for blocks in CHUNKS:
        halves = []
        for side, block in enumerate(blocks):
            row = values[block // 2 : block // 2 + 1]
            halves.append(row if block % 2 == side else pltpu.roll(row, BLOCK, 1))
        if len(halves) == 1:
            halves.append(jnp.full_like(halves[0], -1.0))
        rows.append(jnp.where(lanes < BLOCK, halves[0], halves[1]))
    while len(rows) < 8:
        rows.append(jnp.full_like(rows[0], -1.0))
    return jnp.concatenate(rows, axis=0)


def prepare_kernel(exit_ref, length_ref, order_ref, restore_ref, active_ref, limit_ref, excess_ref):
    upper, shard = seat()
    tall = 2 * BLOCK
    half = BLOCK // 2
    values = chunk_rows(exit_ref[...].astype(jnp.float32))
    deep = (values > 1).astype(jnp.float32)
    rest = ((values >= 0) & (values <= 1)).astype(jnp.float32)
    first = lax.broadcasted_iota(jnp.int32, (tall, tall), 0)
    second = lax.broadcasted_iota(jnp.int32, (tall, tall), 1)
    ahead = (first <= second).astype(jnp.float32)
    counts = jnp.sum(deep, axis=1, keepdims=True)
    excess = jnp.int32(0)
    rank = jnp.where(deep > 0, exact_dot(deep, ahead) - 1, counts + exact_dot(rest, ahead) - 1)
    rank = jnp.where(values >= 0, rank, -1.0).astype(jnp.int32)
    for chunk in range(len(CHUNKS)):
        over = jnp.max(counts[chunk : chunk + 1]) > float(kept_rows(chunk))
        excess = jnp.maximum(excess, over.astype(jnp.int32))
        target = rank[chunk : chunk + 1]
        order = first == target
        order_ref[chunk] = order.astype(jnp.float32).astype(jnp.bfloat16)
        column = jnp.sum(
            jnp.where(first == second, target, 0).astype(jnp.float32), axis=1, keepdims=True
        )
        restore = column.astype(jnp.int32) == second
        restore_ref[chunk] = restore.astype(jnp.float32).astype(jnp.bfloat16)
        natural = (first == second) & (values[chunk : chunk + 1] > 0)
        ranked = order & (deep[chunk : chunk + 1] > 0)
        chosen = jnp.where(upper == 0, natural.astype(jnp.float32), ranked.astype(jnp.float32))
        active_ref[chunk] = jnp.broadcast_to(jnp.sum(chosen, axis=1, keepdims=True), (tall, 128))
    excess_ref[0] = excess
    context = limit_ref.shape[2] // half
    lengths = length_ref[...].astype(jnp.float32)
    lengths = jnp.concatenate([lengths, lengths], axis=0)
    source = lax.broadcasted_iota(jnp.int32, (tall, limit_ref.shape[2]), 0)
    column = lax.broadcasted_iota(jnp.int32, (tall, limit_ref.shape[2]), 1)
    for parity in range(2):
        spread = source == parity * BLOCK + shard * half + column // context
        limit_ref[parity] = exact_dot(lengths, spread.astype(jnp.float32))


def prepare(exits, lengths, context):
    tall = 2 * BLOCK
    count = len(CHUNKS)
    return call(
        prepare_kernel, [exits, lengths], [IN_VMEM] * 2,
        [
            pltpu.VMEM((count, tall, tall), jnp.bfloat16),
            pltpu.VMEM((count, tall, tall), jnp.bfloat16),
            pltpu.VMEM((count, tall, 128), jnp.float32),
            pltpu.VMEM((2, 8, BLOCK // 2 * context), jnp.float32),
            jax.ShapeDtypeStruct((1,), jnp.int32),
        ],
        [IN_VMEM] * 4 + [IN_SMEM],
    )


def own_rows(shard, piece):
    half = BLOCK // 2
    return pl.ds(pl.multiple_of(piece * BLOCK + shard * half, half), half)


def project_kernel(jobs, load, *refs):
    refs = list(refs)
    x_refs = [refs.pop(0) for _ in jobs]
    restore_ref = refs.pop(0) if any(kind != "all" for _, _, kind in jobs) else None
    gain_ref, w_ref = refs.pop(0), refs.pop(0)
    if load == "second":
        other_ref = refs.pop(0)
    keep_ref, keep_sq_ref, send_ref = refs.pop(0), refs.pop(0), refs.pop(0)
    if load:
        held_ref, sem = refs.pop(0), refs.pop()
    if load == "first":
        first_ref = refs.pop(0)
        first_rows = pltpu.make_async_copy(x_refs[0].at[pl.ds(0, first_ref.shape[0])], first_ref, sem.at[8])
        first_rows.start()
        x_refs = [first_ref]
    acc_ref, sq_ref = refs
    _, shard = seat()
    features = w_ref.shape[0]
    pieces = 4 if load == "first" else 2
    depth = features // pieces

    def fetch(i):
        rows = pl.ds(i * depth, depth)
        return pltpu.make_async_copy(w_ref.at[rows], held_ref.at[rows], sem.at[i])

    copies = []
    if load == "first":
        for i in range(pieces):
            fetch(i).start()
    elif load == "second":
        copies = [pltpu.make_async_copy(other_ref, held_ref, sem.at[0])]
    for copy in copies:
        copy.start()

    def multiply(layer, chunk, kind, x_ref):
        tall = len(CHUNKS[chunk]) * BLOCK

        def each(i, carry):
            columns = pl.ds(i * depth if load == "first" else pl.multiple_of(i * depth, depth), depth)
            if kind != "all":
                base = tall // 2 if kind == "rest" else 0
                restore = restore_ref[chunk][:tall, base : base + tall // 2]
                x = jnp.dot(restore, x_ref[:, columns], preferred_element_type=jnp.float32)
            else:
                x = x_ref[:, columns].astype(jnp.float32)
            squares = None
            for lane in range(0, depth, 128):
                part = x[:, lane : lane + 128]
                squares = part * part if squares is None else squares + part * part
            scaled = (x * gain_ref[:, columns].astype(jnp.float32)).astype(jnp.bfloat16)
            if load == "first":
                fetch(i).wait()
                weight = held_ref[columns, :]
            else:
                weight = w_ref[columns, :]
            product = jnp.dot(scaled, weight, preferred_element_type=jnp.float32)
            acc_ref[:tall, :] += product
            sq_ref[:tall, :] += squares
            return carry

        acc_ref[:tall, :] = jnp.zeros((tall, acc_ref.shape[1]), jnp.float32)
        sq_ref[:tall, :] = jnp.zeros((tall, sq_ref.shape[1]), jnp.float32)
        if load == "first":
            for i in range(pieces):
                each(i, 0)
        else:
            lax.fori_loop(0, pieces, each, 0)
        half = BLOCK // 2
        width = keep_ref.shape[1]
        for piece in range(tall // BLOCK):
            here = own_rows(shard, piece)
            there = own_rows(1 - shard, piece)
            rows = pl.ds(piece * half, half)
            keep_ref[rows, :] = acc_ref[here, :]
            send_ref[rows, :width] = acc_ref[there, :].astype(jnp.bfloat16)
            own = jnp.sum(sq_ref[here, :], axis=1, keepdims=True)
            keep_sq_ref[rows, :] = jnp.broadcast_to(own, (half, 128))
            other = jnp.broadcast_to(jnp.sum(sq_ref[there, :], axis=1, keepdims=True), (half, 128))
            high = other.astype(jnp.bfloat16).astype(jnp.float32)
            lanes = lax.broadcasted_iota(jnp.int32, (half, 128), 1)
            send_ref[rows, width:] = jnp.where(lanes < 64, high, other - high).astype(jnp.bfloat16)

    if load == "first":
        first_rows.wait()
    for job, x_ref in zip(jobs, x_refs):
        if load == "first":
            multiply(*job, x_ref)
        else:
            on_layer(job[0], functools.partial(multiply, *job, x_ref))
    if load == "second":
        for copy in copies:
            copy.wait()


def widest(jobs):
    return max(len(CHUNKS[chunk]) for _, chunk, _ in jobs) * BLOCK


def project(jobs, xs, restore, gain, w, load=None, other=None):
    features, width = w.shape
    tall = widest(jobs)
    own = tall // 2
    pooled = any(kind != "all" for _, _, kind in jobs)
    inputs = list(xs) + [restore] * pooled + [gain, w]
    specs = [IN_VMEM] * len(inputs)
    outs = [
        pltpu.VMEM((own, width), jnp.float32),
        pltpu.VMEM((own, 128), jnp.float32),
        pltpu.VMEM((own, width + 128), jnp.bfloat16),
    ]
    scratch = [
        pltpu.VMEM((tall, width), jnp.float32),
        pltpu.VMEM((tall, 128), jnp.float32),
    ]
    if load == "first":
        specs[0] = specs[-1] = IN_HBM
        outs += [pltpu.VMEM(w.shape, w.dtype), pltpu.VMEM((tall, features), jnp.bfloat16)]
        scratch.append(pltpu.SemaphoreType.DMA((9,)))
    elif load == "second":
        inputs.append(other)
        specs.append(IN_HBM)
        outs.append(pltpu.VMEM(other.shape, other.dtype))
        scratch.append(pltpu.SemaphoreType.DMA((1,)))
    return call(
        functools.partial(project_kernel, jobs, load), inputs, specs, outs, scratch=scratch,
        flops=2 * tall * features * width,
    )


def attend_kernel(jobs, total_width, *refs):
    for layer, chunk, _ in jobs:
        on_layer(layer, functools.partial(attend_rows, chunk, total_width, *refs))


def attend_rows(chunk, total_width, keep_ref, keep_sq_ref, recv_ref, kv_ref, limit_ref, out_ref, fit_ref):
    width = keep_ref.shape[1]
    query_width = out_ref.shape[1]
    context = kv_ref.shape[1]
    head_size = kv_ref.shape[2] // 2
    heads = query_width // head_size
    half = BLOCK // 2
    tokens = 16
    columns = tokens * context
    count = len(CHUNKS[chunk]) * half
    other = recv_ref[:count, width:].astype(jnp.float32)
    squares = keep_sq_ref[:count, :1] + other[:, :1] + other[:, 64:65]
    factor = lax.rsqrt(squares / total_width + EPSILON)
    fitted = (keep_ref[:count, :] + recv_ref[:count, :width].astype(jnp.float32)) * factor
    scale = 1.0 / math.sqrt(head_size)
    fit_ref[:count, :query_width] = (fitted[:, :query_width] * scale).astype(jnp.bfloat16)
    fit_ref[:count, query_width:] = fitted[:, query_width:].astype(jnp.bfloat16)
    row = lax.broadcasted_iota(jnp.int32, (heads * tokens, columns), 0)
    column = lax.broadcasted_iota(jnp.int32, (heads * tokens, columns), 1)
    same = (row % tokens) == (column // context)
    position = (lax.broadcasted_iota(jnp.int32, (1, columns), 1) % context).astype(jnp.float32)
    pieces = [
        (place * half + part * tokens, block, part)
        for place, block in enumerate(CHUNKS[chunk])
        for part in range(half // tokens)
    ]
    queries, scores, owns, masks, tops, raws, raw_owns, totals = [], [], [], [], [], [], [], []
    for base, block, part in pieces:
        rows = slice(base, base + tokens)
        queries.append(
            jnp.concatenate(
                [fit_ref[rows, h * head_size : (h + 1) * head_size] for h in range(heads)], axis=0
            )
        )
    for i, (base, block, part) in enumerate(pieces):
        cached = slice(block * half + part * tokens, block * half + (part + 1) * tokens)
        keys = kv_ref[cached, :, :head_size].reshape(columns, head_size)
        scores.append(
            lax.dot_general(
                queries[i], keys, (((1,), (1,)), ((), ())), preferred_element_type=jnp.float32
            )
        )
        key_new = fit_ref[base : base + tokens, query_width : query_width + head_size]
        key_new = jnp.concatenate([key_new.astype(jnp.float32)] * heads, axis=0)
        owns.append(jnp.sum(queries[i].astype(jnp.float32) * key_new, axis=1, keepdims=True))
    for i, (base, block, part) in enumerate(pieces):
        line = block // 2
        limit = limit_ref[block % 2, line : line + 1, part * columns : (part + 1) * columns]
        masks.append(same & (position < limit))
        scores[i] = jnp.where(masks[i], scores[i], NEGATIVE)
        tops.append(jnp.maximum(jnp.max(scores[i], axis=1, keepdims=True), owns[i]))
    for i in range(len(pieces)):
        raws.append(jnp.where(masks[i], jnp.exp(scores[i] - tops[i]), 0.0))
        raw_owns.append(jnp.exp(owns[i] - tops[i]))
        totals.append(jnp.sum(raws[i], axis=1, keepdims=True) + raw_owns[i])
    for i, (base, block, part) in enumerate(pieces):
        rows = slice(base, base + tokens)
        cached = slice(block * half + part * tokens, block * half + (part + 1) * tokens)
        values = kv_ref[cached, :, head_size:].reshape(columns, head_size)
        weights = (raws[i] / totals[i]).astype(jnp.bfloat16)
        own_weight = (raw_owns[i] / totals[i]).astype(jnp.bfloat16).astype(jnp.float32)
        value_new = fit_ref[rows, query_width + head_size :].astype(jnp.float32)
        value_new = jnp.concatenate([value_new] * heads, axis=0)
        attended = jnp.dot(weights, values, preferred_element_type=jnp.float32)
        attended = (attended + own_weight * value_new).astype(jnp.bfloat16)
        for h in range(heads):
            out_ref[rows, h * head_size : (h + 1) * head_size] = attended[
                h * tokens : (h + 1) * tokens
            ]


def attend(jobs, total_width, keep, keep_sq, recv, kv, limits, query_width):
    own = keep.shape[0]
    return call(
        functools.partial(attend_kernel, jobs, total_width),
        [keep, keep_sq, recv, kv, limits], [IN_VMEM] * 5,
        [pltpu.VMEM((own, query_width), jnp.bfloat16)],
        scratch=[pltpu.VMEM((own, keep.shape[1]), jnp.bfloat16)],
        flops=900_000_000,
    )[0]


def output_kernel(jobs, sides, own_ref, recv_ref, active_ref, order_ref, *refs):
    refs = list(refs)
    x_refs = [refs.pop(0) for _ in jobs]
    carry_ref = refs.pop(0) if jobs[-1][0] else None
    w_ref, att_ref = refs.pop(0), refs.pop()
    _, shard = seat()
    half = BLOCK // 2
    tile = 512
    middle = w_ref.shape[1] // 2

    def gather(tall):
        for piece in range(tall // BLOCK):
            rows = pl.ds(piece * half, half)
            att_ref[own_rows(shard, piece), :] = own_ref[rows, :]
            att_ref[own_rows(1 - shard, piece), :] = recv_ref[rows, :]

    def updated(chunk, x_ref, rows, columns, base=0):
        state = x_ref[:, columns].astype(jnp.float32)
        branch = jnp.dot(rows, w_ref[:, columns], preferred_element_type=jnp.float32)[: state.shape[0]]
        active = active_ref[chunk][base : base + state.shape[0], :1] > 0
        return jnp.where(active, state + branch, state).astype(jnp.bfloat16)

    def lower(chunk, x_ref, up_ref, high_rest_ref, low_rest_ref):
        tall = x_ref.shape[0]
        kept = tall // 2
        gather(tall)
        order = order_ref[chunk][:tall, :tall]

        def each(i, carry):
            inner = pl.ds(pl.multiple_of(i * tile, tile), tile)
            for side, rest_ref in enumerate((low_rest_ref, high_rest_ref)):
                columns = pl.ds(pl.multiple_of(i * tile + side * middle, tile), tile)
                state = updated(chunk, x_ref, att_ref[:tall, :], columns)
                ordered = jnp.dot(order, state, preferred_element_type=jnp.float32)
                up_ref[:, columns] = ordered[:kept].astype(jnp.bfloat16)
                rest_ref[:, inner] = ordered[kept:].astype(jnp.bfloat16)
            return carry

        lax.fori_loop(0, middle // tile, each, 0)

    def pooled(chunk, kind, x_ref, *outs):
        kept = x_ref.shape[0]
        tall = 2 * kept
        base = kept if kind == "rest" else 0
        gather(tall)
        rows = jnp.dot(
            order_ref[chunk][base : base + kept, :tall], att_ref[:tall, :], preferred_element_type=jnp.float32
        )
        att_ref[:kept, :] = rows.astype(jnp.bfloat16)

        def each(i, carry):
            inner = pl.ds(pl.multiple_of(i * tile, tile), tile)
            for place, side in enumerate(sides):
                columns = pl.ds(pl.multiple_of(i * tile + side * middle, tile), tile)
                state = updated(chunk, x_ref, att_ref[:tall, :], columns, base)
                if len(outs) < len(sides):
                    outs[0][:, columns] = state
                else:
                    outs[place][:, inner] = state
            return carry

        lax.fori_loop(0, middle // tile, each, 0, unroll=2 if len(sides) == 1 else 1)

    for (layer, chunk, kind), x_ref in zip(jobs, x_refs):
        outs = [refs.pop(0) for _ in range(len(result_shapes(layer, chunk, kind, 2 * middle, sides)))]
        if kind == "all":
            on_layer(layer, functools.partial(lower, chunk, x_ref, *outs))
        else:
            on_layer(layer, functools.partial(pooled, chunk, kind, x_ref, *outs))
        if layer and 0 in sides:
            swap_ref = outs[0]

            def ship():
                swap_ref[...] = carry_ref[...]

            on_layer(0, ship)


def result_shapes(layer, chunk, kind, features, sides):
    kept = kept_rows(chunk)
    whole = pltpu.VMEM((kept, features), jnp.bfloat16)
    part = pltpu.VMEM((kept, features // 2), jnp.bfloat16)
    if layer or kind == "rest":
        return [part] * len(sides)
    return [whole, part, part] if kind == "all" else [whole]


def output(jobs, own, recv, active, order, xs, carry, w, sides=(0, 1)):
    depth, features = w.shape
    outs = []
    for job in jobs:
        outs += result_shapes(*job, features, sides)
    inputs = [own, recv, active, order, *xs] + [carry] * jobs[-1][0] + [w]
    return call(
        functools.partial(output_kernel, jobs, sides), inputs, [IN_VMEM] * len(inputs), outs,
        scratch=[pltpu.VMEM((widest(jobs), depth), jnp.bfloat16)],
        flops=2 * widest(jobs) * features * depth,
    )


def settle_rows(chunk, restore_ref, refs, rows_ref):
    received_ref, own_rest_ref, own_high_ref = refs
    tile = 512
    tall = rows_ref.shape[0]

    def place(first, rest):
        restore = restore_ref[chunk][:tall, :tall]

        def each(i, carry):
            columns = pl.ds(pl.multiple_of(i * tile, tile), tile)
            rows = jnp.concatenate([first[:, columns], rest[:, columns]], axis=0)
            rows_ref[:, columns] = jnp.dot(
                restore, rows, preferred_element_type=jnp.float32
            ).astype(jnp.bfloat16)
            return carry

        lax.fori_loop(0, rows_ref.shape[1] // tile, each, 0)

    on_layer(0, functools.partial(place, received_ref, own_rest_ref))
    on_layer(1, functools.partial(place, own_high_ref, received_ref))


def settle_kernel(jobs, restore_ref, *refs):
    outs = refs[3 * len(jobs) :]
    for i, chunk in enumerate(jobs):
        settle_rows(chunk, restore_ref, refs[3 * i : 3 * i + 3], outs[i])


def settled_shape(chunk, width):
    return pltpu.VMEM((len(CHUNKS[chunk]) * BLOCK, width), jnp.bfloat16)


def settle(jobs, restore, operands):
    width = operands[0].shape[1]
    inputs = [restore, *operands]
    return call(
        functools.partial(settle_kernel, jobs), inputs, [IN_VMEM] * len(inputs),
        [settled_shape(chunk, width) for chunk in jobs],
    )


def finish_kernel(jobs, restore_ref, *refs):
    count = len(CHUNKS) - len(jobs)
    ready, refs = refs[:count], refs[count:]
    operands, refs = refs[: 3 * len(jobs)], refs[3 * len(jobs) :]
    out_ref, rows_refs, sem = refs[0], refs[1:-1], refs[-1]
    started = []

    def put(chunk, rows_ref):
        for i, block in enumerate(CHUNKS[chunk]):
            copy = pltpu.make_async_copy(
                rows_ref.at[pl.ds(i * BLOCK, BLOCK)], out_ref.at[pl.ds(block * BLOCK, BLOCK)], sem.at[block]
            )
            copy.start()
            started.append(copy)

    for chunk in range(count):
        put(chunk, ready[chunk])
    for i, chunk in enumerate(jobs):
        settle_rows(chunk, restore_ref, operands[3 * i : 3 * i + 3], rows_refs[i])
        put(chunk, rows_refs[i])
    for copy in started:
        copy.wait()


def finish(jobs, restore, ready, operands, tokens):
    width = operands[0].shape[1]
    inputs = [restore, *ready, *operands]
    return call(
        functools.partial(finish_kernel, jobs), inputs, [IN_VMEM] * len(inputs),
        [pltpu.HBM((tokens, width), jnp.bfloat16)], [IN_HBM],
        scratch=[settled_shape(chunk, width) for chunk in jobs] + [pltpu.SemaphoreType.DMA((MICRO,))],
    )[0]


def hand_over_kernel(x_ref, out_ref):
    out_ref[...] = x_ref[...]


def hand_over(x):
    return call(hand_over_kernel, [x], [IN_VMEM], [jax.ShapeDtypeStruct(x.shape, x.dtype)])[0]


LAG = 3
SETTLES = ((0, 1), (2,), (3,))


def compact(hidden, exit_layer, lengths, kv_cache, norm_gain, w_qkv, w_out):
    swap = [(i, i ^ 1) for i in range(4)]
    up = [(0, 2), (1, 3)]
    down = [(2, 0), (3, 1)]
    across = [(i, i ^ 2) for i in range(4)]
    query_width = w_out.shape[1]
    total_width = float(2 * w_qkv.shape[1])
    count = len(CHUNKS)

    def send(value, pairs):
        return lax.ppermute(value, "section", pairs)

    order, restore, active, limits, excess = prepare(
        exit_layer.reshape(4, 2 * BLOCK), lengths.reshape(4, 2 * BLOCK), kv_cache.shape[2]
    )
    second, held_cache, *pooled = arrange(hidden[0], order, kv_cache[0])
    moved = [send(value, down) for value in pooled]
    entries = [hidden[0], second] + moved
    kinds = [(0, "all"), (1, "all"), (2, "deep"), (3, "deep"), (2, "rest"), (3, "rest")]
    arrived, settled, own_highs = [], [], []
    high_rests, low_rests = {}, {}
    queue = []

    def exchange(at, jobs, xs, keep, keep_sq, partial):
        received = send(partial, swap)
        own = attend(jobs, total_width, keep, keep_sq, received, held_cache, limits, query_width)
        other = send(own, swap)
        carry = high_rests[at - LAG] if at >= LAG else None
        sides = ((0,), (1,)) if at == count + LAG - 1 else ((0, 1),)
        results = []
        for chosen in sides:
            results += output(
                jobs, own, other, active, order, xs, carry, held_out, chosen
            )
        for layer, chunk, kind in jobs:
            if layer:
                settled.append(send(results.pop(0), across))
                own_highs.append(results.pop(0))
                continue
            if kind != "rest":
                arrived.append(send(results.pop(0), up))
            if kind == "all":
                high_rests[chunk] = results.pop(0)
                low_rests[chunk] = results.pop(0)
            elif kind == "rest":
                low_rests[chunk] = results.pop(0)
                high_rests[chunk] = results.pop(0)

    for at in range(count + LAG):
        jobs, xs = [], []
        if at < len(kinds):
            jobs.append((0, *kinds[at]))
            xs.append(entries[at])
        if at >= LAG:
            jobs.append((1, at - LAG, "deep"))
            xs.append(arrived[at - LAG])
        if at == 0:
            *result, held_proj, first = project(jobs, xs, restore, norm_gain, w_qkv[0], "first")
            xs = [first]
        elif at == 1:
            *result, held_out = project(jobs, xs, restore, norm_gain, held_proj, "second", w_out[0])
        else:
            result = project(jobs, xs, restore, norm_gain, held_proj)
        queue.append((at, jobs, xs, *result))
        if at:
            for item in queue:
                exchange(*item)
            queue = []

    def settle_operands(chunks):
        return [
            value for c in chunks for value in (settled[c], low_rests[c], own_highs[c])
        ]

    ready = []
    for i, chunks in enumerate(SETTLES):
        if i + 1 < len(SETTLES):
            ready += settle(chunks, restore, settle_operands(chunks))
        else:
            out = finish(chunks, restore, ready, settle_operands(chunks), MICRO * BLOCK)
    arguments = (hidden, exit_layer, lengths, kv_cache, norm_gain, w_qkv, w_out)
    return lax.cond(excess[0] > 0, lambda out, *rest: hand_over(body(*rest)), lambda out, *rest: out, out, *arguments)


def solution(mesh):
    paired = mesh.shape["section"] == 4
    return jax.shard_map(
        compact if paired else body,
        mesh=mesh,
        in_specs=(
            P("section", "blk", None),
            P("blk"),
            P("blk"),
            P("section", "blk", None, None),
            P("section", None),
            P("section", None, None),
            P("section", None, None),
        ),
        out_specs=P("blk", "section"),
        check_vma=False,
    )
```
